32 devices in a mesh: rep: 4 (over y, x), col: 8 (over z, core).
Axes of the slice: x: 2, y: 2, z: 4, core: 2. Of those that a mesh axis runs over, the one named last changes fastest.
Arguments:
- tables: float32 [2, 256, 32768], P(None, 'col', 'rep'), may hold values from -4 to 4
- accumulator: float32 [2, 32768], P(None, 'rep'), may hold values from 0.1 to 20
- replica_grads: bfloat16 [4, 2, 256, 16384], P('rep', None, 'col'), may hold values from -6 to 6
- block_ids: int32 [2, 128], replicated, may hold values from 0 to 255, as said below
Outputs:
- new_tables: float32 [2, 256, 32768], P(None, 'col', 'rep')
- new_accumulator: float32 [2, 32768], P(None, 'rep')
The draws below stay inside these ranges and needn't reach their ends.
Inputs may be any that keep to these rules, and one draw needn't show every extreme that they name: `block_ids`: the block ids of one table are distinct; each names a block of 128 rows. Splitting the 32768 rows into 4 equal runs, each run holds exactly 32 of a table's touched blocks.
All inputs are finite; a program needn't handle non-finite values.
Results may differ from the reference program's by a relative error of at most 0.0003.
Values sent between devices are 32-bit elements; how exact they have to be, the bound alone decides.
A program may use at most 64 MiB of HBM per device.

```python
import math
import jax
import jax.numpy as jnp
from jax import lax

DIM = 256
TABLES = 2
BLOCK = 128
ROWS_TAB = 32768
SLAB = 16384
REPS = 4
N_REP = 4


def draw_block_ids(key, part):
    per_shard = ROWS_TAB // BLOCK // N_REP
    taken = SLAB // BLOCK // N_REP
    picked = []
    for table in range(TABLES):
        table_key = jax.random.fold_in(key, 17 + table)
        pieces = []
        for shard in range(N_REP):
            order = jax.random.permutation(jax.random.fold_in(table_key, 1000 + shard), per_shard)
            pieces.append(order[:taken].astype(jnp.int32) + shard * per_shard)
        joined = jnp.concatenate(pieces)
        shuffle = jax.random.permutation(jax.random.fold_in(table_key, 5), SLAB // BLOCK)
        picked.append(joined[shuffle])
    return jnp.stack(picked).astype(jnp.int32)


def levels(own_key, dims, shards, least, high):
    def one(dim, shards_of):
        heights = jax.random.uniform(jax.random.fold_in(jax.random.fold_in(own_key, 6), dim), (shards_of,), jnp.float32, least / len(shards), high / len(shards))
        return jnp.repeat(jnp.exp(heights), dims[dim] // shards_of).reshape((-1,) + (1,) * (len(dims) - dim - 1))

    level = one(*shards[0])
    for cut in shards[1:]:
        level = level * one(*cut)
    return level


def centred(stream_key, dims, deviation, limit, cuts=(), dtype=jnp.bfloat16):
    values = jax.random.normal(stream_key, dims, jnp.float32) * deviation
    if len(cuts) > 0:
        values = levels(stream_key, dims, cuts, -0.22, 0.18) * values
    return jnp.clip(values, min=-limit, max=limit).astype(dtype)


def setup_inputs(seed: int = 0) -> dict:
    arg_keys = jax.random.split(jax.random.key(seed), 5)
    tables = centred(arg_keys[0], (TABLES, DIM, ROWS_TAB), 0.5, 4.0, ((1, 8), (2, 4)), jnp.float32)
    accumulator = jnp.clip(jnp.exp(math.log(20.0) - 5.2983174 * jax.random.uniform(arg_keys[1], (TABLES, ROWS_TAB), jnp.float32) ** levels(arg_keys[1], (TABLES, ROWS_TAB), ((1, 4),), -0.2, 0.2)), 0.1, 20.0)
    replica_grads = centred(arg_keys[2], (REPS, TABLES, DIM, SLAB), 1.0, 6.0, ((0, 4), (2, 8)))
    block_ids = draw_block_ids(jax.random.fold_in(arg_keys[4], 71), 0)
    return dict(tables=tables, accumulator=accumulator, replica_grads=replica_grads, block_ids=block_ids)


def reference(tables, accumulator, replica_grads, block_ids):
    grad = lax.optimization_barrier(jnp.sum(replica_grads.astype(jnp.float32), axis=0))
    squares = lax.optimization_barrier(jnp.sum(grad * grad, axis=1)) / DIM
    nblocks = ROWS_TAB // BLOCK
    outs_tab = []
    outs_acc = []
    for table in range(TABLES):
        ids = block_ids[table].astype(jnp.int32)
        blocked = tables[table].reshape(DIM, nblocks, BLOCK)
        old_rows = jnp.take(blocked, ids, axis=1).reshape(DIM, SLAB)
        acc_blocked = accumulator[table].reshape(nblocks, BLOCK)
        old_accum = jnp.take(acc_blocked, ids, axis=0).reshape(SLAB)
        fresh = old_accum + squares[table]
        moved = old_rows - 0.1 * grad[table] / (jnp.sqrt(fresh)[None, :] + 1e-08)
        blocked = blocked.at[:, ids].set(moved.reshape(DIM, SLAB // BLOCK, BLOCK))
        acc_blocked = acc_blocked.at[ids].set(fresh.reshape(SLAB // BLOCK, BLOCK))
        outs_tab.append(blocked.reshape(DIM, ROWS_TAB))
        outs_acc.append(acc_blocked.reshape(ROWS_TAB))
    return (jnp.stack(outs_tab), jnp.stack(outs_acc))
```

```python
import functools
import math

import jax
import jax.numpy as jnp
from jax import lax
from jax.experimental import pallas as pl
from jax.experimental.pallas import tpu as pltpu
from jax.sharding import PartitionSpec as P

BLOCK = 128
MESH = pl.DeviceIdType.MESH


def cuts(per, last):
    if per % 8:
        return [1] * per
    unit = per // 8
    return [2 * unit] * 2 + [unit] * 4 if last else [2 * unit] * 4


def layout(mesh, shape, n_slab):
    reps, cols = mesh.shape["rep"], mesh.shape["col"]
    inner = math.isqrt(reps)
    while reps % inner:
        inner -= 1
    ntab, width, local_rows = shape
    per = n_slab // BLOCK // reps
    pieces = []
    for t in range(ntab):
        start = 0
        for n in cuts(per, t == ntab - 1):
            pieces.append((t, start, n))
            start += n
    return dict(reps=reps, cols=cols, inner=inner, outer=reps // inner, ntab=ntab, width=width,
                per=per, nblk=n_slab // BLOCK, local=local_rows // BLOCK, dim=width * cols, pieces=pieces)


def lanes(i):
    return pl.ds(i * BLOCK, BLOCK)


def step_kernel(cfg, ids_hbm, grads_hbm, tables_hbm, acc_hbm, image, new_acc, *scratch):
    reps, cols, inner, outer = cfg["reps"], cfg["cols"], cfg["inner"], cfg["outer"]
    ntab, width, per, nblk = cfg["ntab"], cfg["width"], cfg["per"], cfg["nblk"]
    local, dim, pieces = cfg["local"], cfg["dim"], cfg["pieces"]
    n_pieces = len(pieces)
    scratch = list(scratch)

    def take(n):
        out = scratch[:n]
        del scratch[:n]
        return out

    g, totals = take(ntab), take(ntab)
    sq = take(n_pieces)
    (ids_v, order_v, code_v, order_s, code_s, packed, landed, relayed, landed2, acc_slot, step,
     in_sem, meta_sem, s1, r1, s2, r2, s3, r3) = scratch

    me = lax.axis_index("rep")
    my_col = lax.axis_index("col")
    x, y = lax.rem(me, inner), me // inner

    ids_copy = pltpu.make_async_copy(ids_hbm, ids_v, in_sem.at[0])
    ids_copy.start()
    grad_copies = [pltpu.make_async_copy(grads_hbm.at[0, t], g[t], in_sem.at[3 + t]) for t in range(ntab)]
    for copy in grad_copies:
        copy.start()

    barrier = pltpu.get_barrier_semaphore()
    for f in range(1, inner):
        pl.semaphore_signal(barrier, inc=1, device_id={"rep": y * inner + lax.rem(x + f, inner)}, device_id_type=MESH)
    for f in range(1, outer):
        pl.semaphore_signal(barrier, inc=1, device_id={"rep": lax.rem(y + f, outer) * inner + x}, device_id_type=MESH)
    for f in range(1, cols):
        pl.semaphore_signal(barrier, inc=1, device_id={"col": lax.rem(my_col + f, cols)}, device_id_type=MESH)

    acc_copy = pltpu.make_async_copy(acc_hbm, new_acc, in_sem.at[1])
    acc_copy.start()
    table_copy = pltpu.make_async_copy(tables_hbm, image, in_sem.at[2])
    table_copy.start()

    lane = lax.broadcasted_iota(jnp.int32, (nblk, nblk), 1)
    slot = lax.broadcasted_iota(jnp.int32, (nblk, nblk), 0)
    wide = code_v.shape[2]
    own_block = lax.broadcasted_iota(jnp.int32, (nblk, wide), 1) + me * local

    def order_copy(t):
        return pltpu.make_async_copy(order_v.at[t], order_s.at[t], meta_sem.at[0, t])

    def code_copy(t):
        return pltpu.make_async_copy(code_v.at[t], code_s.at[t], meta_sem.at[1, t])

    def rank_blocks(t):
        across = jnp.broadcast_to(ids_v[pl.ds(t, 1), :], (nblk, nblk))
        down = across.T
        place = jnp.sum(jnp.where(down < across, 1, 0), axis=0, keepdims=True)
        hit = jnp.broadcast_to(place, (nblk, nblk)).T == lane
        order = jnp.sum(jnp.where(hit, slot, 0), axis=0, keepdims=True)
        block = jnp.sum(jnp.where(hit, down, 0), axis=0, keepdims=True) - me * local
        order_v[t, pl.ds(0, 1), :] = jnp.clip(order, 0, nblk - 1)
        order_v[t, pl.ds(1, 1), :] = jnp.clip(block, 0, local - 1)
        order_copy(t).start()
        col = jnp.broadcast_to(down[:, :1], (nblk, wide))
        below = jnp.sum(jnp.where(col < own_block, 1, 0), axis=0, keepdims=True) - me * per
        found = jnp.sum(jnp.where(col == own_block, 1, 0), axis=0, keepdims=True)
        code_v[t, pl.ds(0, 1), :] = jnp.where(found > 0, jnp.clip(below, 0, per - 1), -1)
        code_copy(t).start()

    ids_copy.wait()
    for t in range(ntab):
        rank_blocks(t)

    def axes(p):
        return (inner, outer) if p % 2 == 0 else (outer, inner)

    def rank(p, f, s):
        if p % 2 == 0:
            return lax.rem(y + s, outer) * inner + lax.rem(x + f, inner)
        return lax.rem(y + f, outer) * inner + lax.rem(x + s, inner)

    def span(p):
        t, start, n = pieces[p]
        return pl.ds(t * per + start, n)

    def mine(t, owner, i):
        at = order_s[t, 0, owner * per + i]
        return g[t][:, lanes(at)].astype(jnp.float32)

    def first_copy(p, f, s):
        return pltpu.make_async_remote_copy(
            packed.at[f - 1, s, span(p)], landed.at[f - 1, s, span(p)], s1.at[p, f - 1, s], r1.at[p, f - 1, s],
            device_id={"rep": rank(p, f, 0)}, device_id_type=MESH)

    def second_copy(p, s):
        return pltpu.make_async_remote_copy(
            relayed.at[s - 1, span(p)], landed2.at[s - 1, span(p)], s2.at[p, s - 1], r2.at[p, s - 1],
            device_id={"rep": rank(p, 0, s)}, device_id_type=MESH)

    def square_copy(p, f):
        return pltpu.make_async_remote_copy(
            sq[p].at[my_col], sq[p].at[my_col], s3.at[p, f - 1], r3.at[p, f - 1],
            device_id={"col": lax.rem(my_col + f, cols)}, device_id_type=MESH)

    def pack(p, f, s):
        t, start, n = pieces[p]
        owner = rank(p, f, s)
        for i in range(n):
            packed[f - 1, s, t * per + start + i] = mine(t, owner, start + i)
        first_copy(p, f, s).start()

    def send_far(p):
        nf, ns = axes(p)
        for s in range(1, ns):
            for f in range(1, nf):
                pack(p, f, s)

    def send_near(p):
        for f in range(1, axes(p)[0]):
            pack(p, f, 0)

    def relay(p):
        t, start, n = pieces[p]
        nf, ns = axes(p)
        for s in range(1, ns):
            for f in range(1, nf):
                first_copy(p, f, s).wait_recv()
            owner = rank(p, 0, s)
            for i in range(n):
                acc = mine(t, owner, start + i)
                for f in range(1, nf):
                    acc = acc + landed[f - 1, s, t * per + start + i]
                relayed[s - 1, t * per + start + i] = acc
            second_copy(p, s).start()

    def finish(p):
        t, start, n = pieces[p]
        nf, ns = axes(p)
        for f in range(1, nf):
            first_copy(p, f, 0).wait_recv()
        for s in range(1, ns):
            second_copy(p, s).wait_recv()
        for i in range(n):
            acc = mine(t, me, start + i)
            for f in range(1, nf):
                acc = acc + landed[f - 1, 0, t * per + start + i]
            for s in range(1, ns):
                acc = acc + landed2[s - 1, t * per + start + i]
            totals[t][start + i] = acc
            sq[p][my_col, pl.ds(i, 1), :] = jnp.sum(acc * acc, axis=0, keepdims=True)
        for f in range(1, cols):
            square_copy(p, f).start()

    def gather(p):
        t, start, n = pieces[p]
        for f in range(1, cols):
            square_copy(p, f).wait_recv()
        acc = sq[p][0]
        for f in range(1, cols):
            acc = acc + sq[p][f]
        fresh = acc_slot[t, pl.ds(start, n), :] + acc * (1.0 / dim)
        acc_slot[t, pl.ds(start, n), :] = fresh
        step[t, pl.ds(start, n), :] = 0.1 / (jnp.sqrt(fresh) + 1e-8)
        for i in range(start, start + n):
            totals[t][i] = totals[t][i] * step[t, pl.ds(i, 1), :]

    def place(t):
        for b in range(local):
            code = code_s[t, 0, b]
            at = jnp.maximum(code, 0)
            where = pl.ds(b * BLOCK, BLOCK)
            hit = jnp.full((width, BLOCK), code, jnp.int32) >= 0
            old = image[t, :, where]
            image[t, :, where] = jnp.where(hit, old - totals[t][at], old)
            old_acc = new_acc[pl.ds(t, 1), where]
            new_acc[pl.ds(t, 1), where] = jnp.where(hit[:1], acc_slot[t, pl.ds(at, 1), :], old_acc)

    for t in range(ntab):
        order_copy(t).wait()
        grad_copies[t].wait()
        if t == 0:
            pl.semaphore_wait(barrier, inner - 1 + outer - 1 + cols - 1)
        for p in range(n_pieces):
            if pieces[p][0] == t:
                send_far(p)
    for p in range(n_pieces):
        send_near(p)

    acc_copy.wait()
    for t in range(ntab):
        for i in range(per):
            block = order_s[t, 1, me * per + i]
            acc_slot[t, pl.ds(i, 1), :] = new_acc[pl.ds(t, 1), lanes(block)]

    for p in range(n_pieces):
        relay(p)
    table_copy.wait()
    for t in range(ntab):
        code_copy(t).wait()
    for p in range(n_pieces + 1):
        if p < n_pieces:
            finish(p)
        if p > 0:
            gather(p - 1)
            t = pieces[p - 1][0]
            if p == n_pieces or pieces[p][0] != t:
                place(t)

    for p in range(n_pieces):
        nf, ns = axes(p)
        for s in range(ns):
            for f in range(1, nf):
                first_copy(p, f, s).wait_send()
        for s in range(1, ns):
            second_copy(p, s).wait_send()
        for f in range(1, cols):
            square_copy(p, f).wait_send()


def store_kernel(image, acc, tables_out, acc_out, sem, acc_sem):
    copies = [pltpu.make_async_copy(acc, acc_out, acc_sem)]
    for t in range(image.shape[0]):
        for d in range(image.shape[1] // 8):
            rows = pl.ds(d * 8, 8)
            copies.append(pltpu.make_async_copy(image.at[t, rows], tables_out.at[t, rows], sem.at[t, d]))
    for copy in copies:
        copy.start()
    for copy in copies:
        copy.wait()


def body(mesh, tables, accumulator, replica_grads, block_ids):
    cfg = layout(mesh, tables.shape, replica_grads.shape[3])
    ntab, width, per, nblk = cfg["ntab"], cfg["width"], cfg["per"], cfg["nblk"]
    cols, pieces = cfg["cols"], cfg["pieces"]
    side = max(cfg["inner"], cfg["outer"])
    slots, n_pieces = ntab * per, len(pieces)
    wide = -(-cfg["local"] // BLOCK) * BLOCK
    f32, i32 = jnp.float32, jnp.int32
    dma = pltpu.SemaphoreType.DMA
    hbm = pl.BlockSpec(memory_space=pltpu.HBM)
    vmem = pl.BlockSpec(memory_space=pltpu.VMEM)
    image, new_acc = pl.pallas_call(
        functools.partial(step_kernel, cfg),
        out_shape=(jax.ShapeDtypeStruct(tables.shape, f32), jax.ShapeDtypeStruct(accumulator.shape, f32)),
        in_specs=[hbm] * 4,
        out_specs=(vmem, vmem),
        scratch_shapes=[
            *[pltpu.VMEM(replica_grads.shape[2:], replica_grads.dtype) for _ in range(ntab)],
            *[pltpu.VMEM((per, width, BLOCK), f32) for _ in range(ntab)],
            *[pltpu.VMEM((cols, n, BLOCK), f32) for _, _, n in pieces],
            pltpu.VMEM(block_ids.shape, i32),
            pltpu.VMEM((ntab, 2, nblk), i32),
            pltpu.VMEM((ntab, 1, wide), i32),
            pltpu.SMEM((ntab, 2, nblk), i32),
            pltpu.SMEM((ntab, 1, wide), i32),
            pltpu.VMEM((side - 1, side, slots, width, BLOCK), f32),
            pltpu.VMEM((side - 1, side, slots, width, BLOCK), f32),
            pltpu.VMEM((side - 1, slots, width, BLOCK), f32),
            pltpu.VMEM((side - 1, slots, width, BLOCK), f32),
            pltpu.VMEM((ntab, per, BLOCK), f32),
            pltpu.VMEM((ntab, per, BLOCK), f32),
            dma((3 + ntab,)), dma((2, ntab)),
            dma((n_pieces, side - 1, side)), dma((n_pieces, side - 1, side)),
            dma((n_pieces, side - 1)), dma((n_pieces, side - 1)),
            dma((n_pieces, cols - 1)), dma((n_pieces, cols - 1)),
        ],
        compiler_params=pltpu.CompilerParams(
            collective_id=0, has_side_effects=True, vmem_limit_bytes=32 * 2**20),
        name="exchange",
    )(*[pltpu.with_memory_space_constraint(a, pltpu.HBM) for a in (block_ids, replica_grads, tables, accumulator)])
    return pl.pallas_call(
        store_kernel,
        out_shape=(jax.ShapeDtypeStruct(tables.shape, f32), jax.ShapeDtypeStruct(accumulator.shape, f32)),
        in_specs=[vmem, vmem],
        out_specs=(hbm, hbm),
        scratch_shapes=[dma((ntab, width // 8)), dma(())],
        compiler_params=pltpu.CompilerParams(vmem_limit_bytes=2**20),
        name="store",
    )(image, new_acc)


def solution(mesh):
    return jax.shard_map(
        functools.partial(body, mesh),
        mesh=mesh,
        in_specs=(P(None, "col", "rep"), P(None, "rep"), P("rep", None, "col", None), P()),
        out_specs=(P(None, "col", "rep"), P(None, "rep")),
        check_vma=False,
    )
```

```python
import functools
import math

import jax
import jax.numpy as jnp
from jax import lax
from jax.experimental import pallas as pl
from jax.experimental.pallas import tpu as pltpu
from jax.sharding import PartitionSpec as P

BLOCK = 128
MESH = pl.DeviceIdType.MESH


def cuts(per, last):
    if per % 8:
        return [1] * per
    unit = per // 8
    return [2 * unit] * 2 + [unit] * 4 if last else [2 * unit] * 4


def layout(mesh, shape, n_slab):
    reps, cols = mesh.shape["rep"], mesh.shape["col"]
    inner = math.isqrt(reps)
    while reps % inner:
        inner -= 1
    ntab, width, local_rows = shape
    per = n_slab // BLOCK // reps
    pieces = []
    for t in range(ntab):
        start = 0
        for n in cuts(per, t == ntab - 1):
            pieces.append((t, start, n))
            start += n
    return dict(reps=reps, cols=cols, inner=inner, outer=reps // inner, ntab=ntab, width=width,
                per=per, nblk=n_slab // BLOCK, local=local_rows // BLOCK, dim=width * cols, pieces=pieces)


def lanes(i):
    return pl.ds(i * BLOCK, BLOCK)


def step_kernel(cfg, ids_hbm, grads_hbm, tables_hbm, acc_hbm, image, new_acc, *scratch):
    reps, cols, inner, outer = cfg["reps"], cfg["cols"], cfg["inner"], cfg["outer"]
    ntab, width, per, nblk = cfg["ntab"], cfg["width"], cfg["per"], cfg["nblk"]
    local, dim, pieces = cfg["local"], cfg["dim"], cfg["pieces"]
    n_pieces = len(pieces)
    scratch = list(scratch)

    def take(n):
        out = scratch[:n]
        del scratch[:n]
        return out

    g, totals = take(ntab), take(ntab)
    sq = take(n_pieces)
    (ids_v, order_v, code_v, order_s, code_s, packed, landed, relayed, landed2, acc_slot, step,
     in_sem, meta_sem, s1, r1, s2, r2, s3, r3) = scratch

    me = lax.axis_index("rep")
    my_col = lax.axis_index("col")
    x, y = lax.rem(me, inner), me // inner

    ids_copy = pltpu.make_async_copy(ids_hbm, ids_v, in_sem.at[0])
    ids_copy.start()
    grad_copies = [pltpu.make_async_copy(grads_hbm.at[0, t], g[t], in_sem.at[3 + t]) for t in range(ntab)]
    for copy in grad_copies:
        copy.start()

    barrier = pltpu.get_barrier_semaphore()
    for f in range(1, inner):
        pl.semaphore_signal(barrier, inc=1, device_id={"rep": y * inner + lax.rem(x + f, inner)}, device_id_type=MESH)
    for f in range(1, outer):
        pl.semaphore_signal(barrier, inc=1, device_id={"rep": lax.rem(y + f, outer) * inner + x}, device_id_type=MESH)
    for f in range(1, cols):
        pl.semaphore_signal(barrier, inc=1, device_id={"col": lax.rem(my_col + f, cols)}, device_id_type=MESH)

    acc_copy = pltpu.make_async_copy(acc_hbm, new_acc, in_sem.at[1])
    acc_copy.start()
    table_copy = pltpu.make_async_copy(tables_hbm, image, in_sem.at[2])
    table_copy.start()

    lane = lax.broadcasted_iota(jnp.int32, (nblk, nblk), 1)
    slot = lax.broadcasted_iota(jnp.int32, (nblk, nblk), 0)
    wide = code_v.shape[2]
    own_block = lax.broadcasted_iota(jnp.int32, (nblk, wide), 1) + me * local

    def order_copy(t):
        return pltpu.make_async_copy(order_v.at[t], order_s.at[t], meta_sem.at[0, t])

    def code_copy(t):
        return pltpu.make_async_copy(code_v.at[t], code_s.at[t], meta_sem.at[1, t])

    def rank_blocks(t):
        across = jnp.broadcast_to(ids_v[pl.ds(t, 1), :], (nblk, nblk))
        down = across.T
        place = jnp.sum(jnp.where(down < across, 1, 0), axis=0, keepdims=True)
        hit = jnp.broadcast_to(place, (nblk, nblk)).T == lane
        order = jnp.sum(jnp.where(hit, slot, 0), axis=0, keepdims=True)
        block = jnp.sum(jnp.where(hit, down, 0), axis=0, keepdims=True) - me * local
        order_v[t, pl.ds(0, 1), :] = jnp.clip(order, 0, nblk - 1)
        order_v[t, pl.ds(1, 1), :] = jnp.clip(block, 0, local - 1)
        order_copy(t).start()
        col = jnp.broadcast_to(down[:, :1], (nblk, wide))
        below = jnp.sum(jnp.where(col < own_block, 1, 0), axis=0, keepdims=True) - me * per
        found = jnp.sum(jnp.where(col == own_block, 1, 0), axis=0, keepdims=True)
        code_v[t, pl.ds(0, 1), :] = jnp.where(found > 0, jnp.clip(below, 0, per - 1), -1)
        code_copy(t).start()

    ids_copy.wait()
    rank_blocks(0)

    def axes(p):
        return (inner, outer) if p % 2 == 0 else (outer, inner)

    def rank(p, f, s):
        if p % 2 == 0:
            return lax.rem(y + s, outer) * inner + lax.rem(x + f, inner)
        return lax.rem(y + f, outer) * inner + lax.rem(x + s, inner)

    def span(p):
        t, start, n = pieces[p]
        return pl.ds(t * per + start, n)

    def mine(t, owner, i):
        at = order_s[t, 0, owner * per + i]
        return g[t][:, lanes(at)].astype(jnp.float32)

    def first_copy(p, f, s):
        return pltpu.make_async_remote_copy(
            packed.at[f - 1, s, span(p)], landed.at[f - 1, s, span(p)], s1.at[p, f - 1, s], r1.at[p, f - 1, s],
            device_id={"rep": rank(p, f, 0)}, device_id_type=MESH)

    def second_copy(p, s):
        return pltpu.make_async_remote_copy(
            relayed.at[s - 1, span(p)], landed2.at[s - 1, span(p)], s2.at[p, s - 1], r2.at[p, s - 1],
            device_id={"rep": rank(p, 0, s)}, device_id_type=MESH)

    def square_copy(p, f):
        return pltpu.make_async_remote_copy(
            sq[p].at[my_col], sq[p].at[my_col], s3.at[p, f - 1], r3.at[p, f - 1],
            device_id={"col": lax.rem(my_col + f, cols)}, device_id_type=MESH)

    def pack(p, f, s):
        t, start, n = pieces[p]
        owner = rank(p, f, s)
        for i in range(n):
            packed[f - 1, s, t * per + start + i] = mine(t, owner, start + i)
        first_copy(p, f, s).start()

    def send_far(p):
        nf, ns = axes(p)
        for s in range(1, ns):
            for f in range(1, nf):
                pack(p, f, s)

    def send_near(p):
        for f in range(1, axes(p)[0]):
            pack(p, f, 0)

    def relay(p):
        t, start, n = pieces[p]
        nf, ns = axes(p)
        for s in range(1, ns):
            for f in range(1, nf):
                first_copy(p, f, s).wait_recv()
            owner = rank(p, 0, s)
            for i in range(n):
                acc = mine(t, owner, start + i)
                for f in range(1, nf):
                    acc = acc + landed[f - 1, s, t * per + start + i]
                relayed[s - 1, t * per + start + i] = acc
            second_copy(p, s).start()

    def finish(p):
        t, start, n = pieces[p]
        nf, ns = axes(p)
        for f in range(1, nf):
            first_copy(p, f, 0).wait_recv()
        for s in range(1, ns):
            second_copy(p, s).wait_recv()
        for i in range(n):
            acc = mine(t, me, start + i)
            for f in range(1, nf):
                acc = acc + landed[f - 1, 0, t * per + start + i]
            for s in range(1, ns):
                acc = acc + landed2[s - 1, t * per + start + i]
            totals[t][start + i] = acc
            sq[p][my_col, pl.ds(i, 1), :] = jnp.sum(acc * acc, axis=0, keepdims=True)
        for f in range(1, cols):
            square_copy(p, f).start()

    def gather(p):
        t, start, n = pieces[p]
        for f in range(1, cols):
            square_copy(p, f).wait_recv()
        acc = sq[p][0]
        for f in range(1, cols):
            acc = acc + sq[p][f]
        fresh = acc_slot[t, pl.ds(start, n), :] + acc * (1.0 / dim)
        acc_slot[t, pl.ds(start, n), :] = fresh
        step[t, pl.ds(start, n), :] = 0.1 / (jnp.sqrt(fresh) + 1e-8)
        for i in range(start, start + n):
            totals[t][i] = totals[t][i] * step[t, pl.ds(i, 1), :]

    def place(t):
        for b in range(local):
            code = code_s[t, 0, b]
            at = jnp.maximum(code, 0)
            where = pl.ds(b * BLOCK, BLOCK)
            hit = jnp.full((width, BLOCK), code, jnp.int32) >= 0
            old = image[t, :, where]
            image[t, :, where] = jnp.where(hit, old - totals[t][at], old)
            old_acc = new_acc[pl.ds(t, 1), where]
            new_acc[pl.ds(t, 1), where] = jnp.where(hit[:1], acc_slot[t, pl.ds(at, 1), :], old_acc)

    for t in range(ntab):
        order_copy(t).wait()
        grad_copies[t].wait()
        if t == 0:
            pl.semaphore_wait(barrier, inner - 1 + outer - 1 + cols - 1)
        for p in range(n_pieces):
            if pieces[p][0] == t:
                send_far(p)
        if t + 1 < ntab:
            rank_blocks(t + 1)
    for p in range(n_pieces):
        send_near(p)

    acc_copy.wait()
    for t in range(ntab):
        for i in range(per):
            block = order_s[t, 1, me * per + i]
            acc_slot[t, pl.ds(i, 1), :] = new_acc[pl.ds(t, 1), lanes(block)]

    for p in range(n_pieces):
        relay(p)
    table_copy.wait()
    for t in range(ntab):
        code_copy(t).wait()
    for p in range(n_pieces):
        finish(p)
    for p in range(n_pieces):
        gather(p)
        t = pieces[p][0]
        if p + 1 == n_pieces or pieces[p + 1][0] != t:
            place(t)

    for p in range(n_pieces):
        nf, ns = axes(p)
        for s in range(ns):
            for f in range(1, nf):
                first_copy(p, f, s).wait_send()
        for s in range(1, ns):
            second_copy(p, s).wait_send()
        for f in range(1, cols):
            square_copy(p, f).wait_send()


def store_kernel(image, acc, tables_out, acc_out, sem, acc_sem):
    copies = [pltpu.make_async_copy(acc, acc_out, acc_sem)]
    for t in range(image.shape[0]):
        for d in range(image.shape[1] // 8):
            rows = pl.ds(d * 8, 8)
            copies.append(pltpu.make_async_copy(image.at[t, rows], tables_out.at[t, rows], sem.at[t, d]))
    for copy in copies:
        copy.start()
    for copy in copies:
        copy.wait()


def body(mesh, tables, accumulator, replica_grads, block_ids):
    cfg = layout(mesh, tables.shape, replica_grads.shape[3])
    ntab, width, per, nblk = cfg["ntab"], cfg["width"], cfg["per"], cfg["nblk"]
    cols, pieces = cfg["cols"], cfg["pieces"]
    side = max(cfg["inner"], cfg["outer"])
    slots, n_pieces = ntab * per, len(pieces)
    wide = -(-cfg["local"] // BLOCK) * BLOCK
    f32, i32 = jnp.float32, jnp.int32
    dma = pltpu.SemaphoreType.DMA
    hbm = pl.BlockSpec(memory_space=pltpu.HBM)
    vmem = pl.BlockSpec(memory_space=pltpu.VMEM)
    image, new_acc = pl.pallas_call(
        functools.partial(step_kernel, cfg),
        out_shape=(jax.ShapeDtypeStruct(tables.shape, f32), jax.ShapeDtypeStruct(accumulator.shape, f32)),
        in_specs=[hbm] * 4,
        out_specs=(vmem, vmem),
        scratch_shapes=[
            *[pltpu.VMEM(replica_grads.shape[2:], replica_grads.dtype) for _ in range(ntab)],
            *[pltpu.VMEM((per, width, BLOCK), f32) for _ in range(ntab)],
            *[pltpu.VMEM((cols, n, BLOCK), f32) for _, _, n in pieces],
            pltpu.VMEM(block_ids.shape, i32),
            pltpu.VMEM((ntab, 2, nblk), i32),
            pltpu.VMEM((ntab, 1, wide), i32),
            pltpu.SMEM((ntab, 2, nblk), i32),
            pltpu.SMEM((ntab, 1, wide), i32),
            pltpu.VMEM((side - 1, side, slots, width, BLOCK), f32),
            pltpu.VMEM((side - 1, side, slots, width, BLOCK), f32),
            pltpu.VMEM((side - 1, slots, width, BLOCK), f32),
            pltpu.VMEM((side - 1, slots, width, BLOCK), f32),
            pltpu.VMEM((ntab, per, BLOCK), f32),
            pltpu.VMEM((ntab, per, BLOCK), f32),
            dma((3 + ntab,)), dma((2, ntab)),
            dma((n_pieces, side - 1, side)), dma((n_pieces, side - 1, side)),
            dma((n_pieces, side - 1)), dma((n_pieces, side - 1)),
            dma((n_pieces, cols - 1)), dma((n_pieces, cols - 1)),
        ],
        compiler_params=pltpu.CompilerParams(
            collective_id=0, has_side_effects=True, vmem_limit_bytes=32 * 2**20),
        name="exchange",
    )(*[pltpu.with_memory_space_constraint(a, pltpu.HBM) for a in (block_ids, replica_grads, tables, accumulator)])
    return pl.pallas_call(
        store_kernel,
        out_shape=(jax.ShapeDtypeStruct(tables.shape, f32), jax.ShapeDtypeStruct(accumulator.shape, f32)),
        in_specs=[vmem, vmem],
        out_specs=(hbm, hbm),
        scratch_shapes=[dma((ntab, width // 8)), dma(())],
        compiler_params=pltpu.CompilerParams(vmem_limit_bytes=2**20),
        name="store",
    )(image, new_acc)


def solution(mesh):
    return jax.shard_map(
        functools.partial(body, mesh),
        mesh=mesh,
        in_specs=(P(None, "col", "rep"), P(None, "rep"), P("rep", None, "col", None), P()),
        out_specs=(P(None, "col", "rep"), P(None, "rep")),
        check_vma=False,
    )
```

```python
import functools
import math

import jax
import jax.numpy as jnp
from jax import lax
from jax.experimental import pallas as pl
from jax.experimental.pallas import tpu as pltpu
from jax.sharding import PartitionSpec as P

BLOCK = 128
MESH = pl.DeviceIdType.MESH


def cuts(per, last):
    if per % 8:
        return [1] * per
    unit = per // 8
    return [2 * unit] * 2 + [unit] * 4 if last else [2 * unit] * 4


def layout(mesh, shape, n_slab):
    reps, cols = mesh.shape["rep"], mesh.shape["col"]
    inner = math.isqrt(reps)
    while reps % inner:
        inner -= 1
    ntab, width, local_rows = shape
    per = n_slab // BLOCK // reps
    pieces = []
    for t in range(ntab):
        start = 0
        for n in cuts(per, t == ntab - 1):
            pieces.append((t, start, n))
            start += n
    return dict(reps=reps, cols=cols, inner=inner, outer=reps // inner, ntab=ntab, width=width,
                per=per, nblk=n_slab // BLOCK, local=local_rows // BLOCK, dim=width * cols, pieces=pieces)


def lanes(i):
    return pl.ds(i * BLOCK, BLOCK)


def step_kernel(cfg, ids_hbm, grads_hbm, tables_hbm, acc_hbm, image, new_acc, *scratch):
    reps, cols, inner, outer = cfg["reps"], cfg["cols"], cfg["inner"], cfg["outer"]
    ntab, width, per, nblk = cfg["ntab"], cfg["width"], cfg["per"], cfg["nblk"]
    local, dim, pieces = cfg["local"], cfg["dim"], cfg["pieces"]
    n_pieces = len(pieces)
    scratch = list(scratch)

    def take(n):
        out = scratch[:n]
        del scratch[:n]
        return out

    g, totals = take(ntab), take(ntab)
    sq = take(n_pieces)
    (ids_v, order_v, code_v, order_s, code_s, packed, landed, relayed, arrived, acc_slot, step, sent,
     in_sem, meta_sem, send_sem, far_sem, own_sem, sq_sem, up, down) = scratch

    me = lax.axis_index("rep")
    my_col = lax.axis_index("col")
    x, y = lax.rem(me, inner), me // inner

    ids_copy = pltpu.make_async_copy(ids_hbm, ids_v, in_sem.at[0])
    ids_copy.start()
    grad_copies = [pltpu.make_async_copy(grads_hbm.at[0, t], g[t], in_sem.at[3 + t]) for t in range(ntab)]
    for copy in grad_copies:
        copy.start()

    barrier = pltpu.get_barrier_semaphore()
    for f in range(1, inner):
        pl.semaphore_signal(barrier, inc=1, device_id={"rep": y * inner + lax.rem(x + f, inner)}, device_id_type=MESH)
    for f in range(1, outer):
        pl.semaphore_signal(barrier, inc=1, device_id={"rep": lax.rem(y + f, outer) * inner + x}, device_id_type=MESH)

    def pass_on(sem, way):
        pl.semaphore_signal(sem, inc=1, device_id={"col": my_col + way}, device_id_type=MESH)

    pl.when(my_col > 0)(lambda: pass_on(barrier, -1))
    pl.when(my_col < cols - 1)(lambda: pass_on(barrier, 1))

    acc_copy = pltpu.make_async_copy(acc_hbm, new_acc, in_sem.at[1])
    acc_copy.start()
    table_copy = pltpu.make_async_copy(tables_hbm, image, in_sem.at[2])
    table_copy.start()

    lane = lax.broadcasted_iota(jnp.int32, (nblk, nblk), 1)
    slot = lax.broadcasted_iota(jnp.int32, (nblk, nblk), 0)
    wide = code_v.shape[2]
    own_block = lax.broadcasted_iota(jnp.int32, (nblk, wide), 1) + me * local

    def order_copy(t):
        return pltpu.make_async_copy(order_v.at[t], order_s.at[t], meta_sem.at[0, t])

    def code_copy(t):
        return pltpu.make_async_copy(code_v.at[t], code_s.at[t], meta_sem.at[1, t])

    def rank_blocks(t):
        across = jnp.broadcast_to(ids_v[pl.ds(t, 1), :], (nblk, nblk))
        down = across.T
        place = jnp.sum(jnp.where(down < across, 1, 0), axis=0, keepdims=True)
        hit = jnp.broadcast_to(place, (nblk, nblk)).T == lane
        order = jnp.sum(jnp.where(hit, slot, 0), axis=0, keepdims=True)
        block = jnp.sum(jnp.where(hit, down, 0), axis=0, keepdims=True) - me * local
        order_v[t, pl.ds(0, 1), :] = jnp.clip(order, 0, nblk - 1)
        order_v[t, pl.ds(1, 1), :] = jnp.clip(block, 0, local - 1)
        order_copy(t).start()
        col = jnp.broadcast_to(down[:, :1], (nblk, wide))
        below = jnp.sum(jnp.where(col < own_block, 1, 0), axis=0, keepdims=True) - me * per
        found = jnp.sum(jnp.where(col == own_block, 1, 0), axis=0, keepdims=True)
        code_v[t, pl.ds(0, 1), :] = jnp.where(found > 0, jnp.clip(below, 0, per - 1), -1)
        code_copy(t).start()

    ids_copy.wait()
    rank_blocks(0)

    def axes(p):
        return (inner, outer) if p % 2 == 0 else (outer, inner)

    def rank(p, f, s):
        if p % 2 == 0:
            return lax.rem(y + s, outer) * inner + lax.rem(x + f, inner)
        return lax.rem(y + f, outer) * inner + lax.rem(x + s, inner)

    def span(p):
        t, start, n = pieces[p]
        return pl.ds(t * per + start, n)

    def mine(t, owner, i):
        at = order_s[t, 0, owner * per + i]
        return g[t][:, lanes(at)].astype(jnp.float32)

    def first_copy(p, f, s):
        here = arrived.at[f - 1, span(p)] if s == 0 else landed.at[f - 1, s - 1, span(p)]
        return pltpu.make_async_remote_copy(
            packed.at[f - 1, s, span(p)], here, send_sem.at[0], own_sem.at[p] if s == 0 else far_sem.at[p],
            device_id={"rep": rank(p, f, 0)}, device_id_type=MESH)

    def second_copy(p, s):
        nf = axes(p)[0]
        return pltpu.make_async_remote_copy(
            relayed.at[s - 1, span(p)], arrived.at[nf - 2 + s, span(p)], send_sem.at[1], own_sem.at[p],
            device_id={"rep": rank(p, 0, s)}, device_id_type=MESH)

    def square_copy(p, f):
        return pltpu.make_async_remote_copy(
            sq[p].at[my_col], sq[p].at[my_col], send_sem.at[2], sq_sem.at[p],
            device_id={"col": lax.rem(my_col + f, cols)}, device_id_type=MESH)

    def wait_all(ref, sem):
        pltpu.make_async_copy(ref, ref, sem).wait()

    def pack(p, f, s):
        t, start, n = pieces[p]
        owner = rank(p, f, s)
        for i in range(n):
            packed[f - 1, s, t * per + start + i] = mine(t, owner, start + i)
        first_copy(p, f, s).start()

    def send_far(p):
        nf, ns = axes(p)
        for s in range(1, ns):
            for f in range(1, nf):
                pack(p, f, s)

    def send_near(p):
        for f in range(1, axes(p)[0]):
            pack(p, f, 0)

    def relay(p):
        t, start, n = pieces[p]
        nf, ns = axes(p)
        wait_all(landed.at[pl.ds(0, nf - 1), pl.ds(0, ns - 1), span(p)], far_sem.at[p])
        for s in range(1, ns):
            owner = rank(p, 0, s)
            for i in range(n):
                acc = mine(t, owner, start + i)
                for f in range(1, nf):
                    acc = acc + landed[f - 1, s - 1, t * per + start + i]
                relayed[s - 1, t * per + start + i] = acc
            second_copy(p, s).start()

    def finish(p):
        t, start, n = pieces[p]
        nf, ns = axes(p)
        wait_all(arrived.at[pl.ds(0, nf + ns - 2), span(p)], own_sem.at[p])
        for i in range(n):
            acc = mine(t, me, start + i)
            for k in range(nf + ns - 2):
                acc = acc + arrived[k, t * per + start + i]
            totals[t][start + i] = acc
            sq[p][my_col, pl.ds(i, 1), :] = jnp.sum(acc * acc, axis=0, keepdims=True)
        for f in range(1, cols):
            square_copy(p, f).start()

    def gather(p):
        t, start, n = pieces[p]
        wait_all(sq[p].at[pl.ds(0, cols - 1)], sq_sem.at[p])
        acc = sq[p][0]
        for f in range(1, cols):
            acc = acc + sq[p][f]
        fresh = acc_slot[t, pl.ds(start, n), :] + acc * (1.0 / dim)
        acc_slot[t, pl.ds(start, n), :] = fresh
        step[t, pl.ds(start, n), :] = 0.1 / (jnp.sqrt(fresh) + 1e-8)
        for i in range(start, start + n):
            totals[t][i] = totals[t][i] * step[t, pl.ds(i, 1), :]

    def place(t):
        for b in range(local):
            code = code_s[t, 0, b]
            at = jnp.maximum(code, 0)
            where = pl.ds(b * BLOCK, BLOCK)
            hit = jnp.full((width, BLOCK), code, jnp.int32) >= 0
            old = image[t, :, where]
            image[t, :, where] = jnp.where(hit, old - totals[t][at], old)
            old_acc = new_acc[pl.ds(t, 1), where]
            new_acc[pl.ds(t, 1), where] = jnp.where(hit[:1], acc_slot[t, pl.ds(at, 1), :], old_acc)

    def sweep(sem, way, behind, ahead):
        pl.when(behind)(lambda: pl.semaphore_wait(sem, 1))
        pl.when(ahead)(lambda: pass_on(sem, way))

    for t in range(ntab):
        order_copy(t).wait()
        grad_copies[t].wait()
        if t == 0:
            beside = jnp.minimum(my_col, 1) + jnp.minimum(cols - 1 - my_col, 1)
            pl.semaphore_wait(barrier, inner - 1 + outer - 1 + beside)
        for p in range(n_pieces):
            if pieces[p][0] == t:
                send_far(p)
        if t + 1 < ntab:
            rank_blocks(t + 1)
    for p in range(n_pieces):
        send_near(p)

    acc_copy.wait()
    for t in range(ntab):
        for i in range(per):
            block = order_s[t, 1, me * per + i]
            acc_slot[t, pl.ds(i, 1), :] = new_acc[pl.ds(t, 1), lanes(block)]

    for p in range(n_pieces):
        relay(p)
    sweep(up, 1, my_col > 0, my_col < cols - 1)
    sweep(down, -1, my_col < cols - 1, my_col > 0)
    table_copy.wait()
    for t in range(ntab):
        code_copy(t).wait()
    for p in range(n_pieces):
        finish(p)
    for p in range(n_pieces):
        gather(p)
        t = pieces[p][0]
        if p + 1 == n_pieces or pieces[p + 1][0] != t:
            place(t)

    if inner == outer:
        wait_all(packed, send_sem.at[0])
        wait_all(relayed, send_sem.at[1])
    else:
        for p in range(n_pieces):
            nf, ns = axes(p)
            wait_all(packed.at[pl.ds(0, nf - 1), pl.ds(0, ns), span(p)], send_sem.at[0])
            wait_all(relayed.at[pl.ds(0, ns - 1), span(p)], send_sem.at[1])
    wait_all(sent, send_sem.at[2])


def store_kernel(image, acc, tables_out, acc_out, sem, acc_sem):
    copies = [pltpu.make_async_copy(acc, acc_out, acc_sem)]
    for t in range(image.shape[0]):
        for d in range(image.shape[1] // 8):
            rows = pl.ds(d * 8, 8)
            copies.append(pltpu.make_async_copy(image.at[t, rows], tables_out.at[t, rows], sem.at[t, d]))
    for copy in copies:
        copy.start()
    for copy in copies:
        copy.wait()


def body(mesh, tables, accumulator, replica_grads, block_ids):
    cfg = layout(mesh, tables.shape, replica_grads.shape[3])
    ntab, width, per, nblk = cfg["ntab"], cfg["width"], cfg["per"], cfg["nblk"]
    cols, pieces = cfg["cols"], cfg["pieces"]
    side = max(cfg["inner"], cfg["outer"])
    slots, n_pieces = ntab * per, len(pieces)
    wide = -(-cfg["local"] // BLOCK) * BLOCK
    f32, i32 = jnp.float32, jnp.int32
    dma = pltpu.SemaphoreType.DMA
    hbm = pl.BlockSpec(memory_space=pltpu.HBM)
    vmem = pl.BlockSpec(memory_space=pltpu.VMEM)
    image, new_acc = pl.pallas_call(
        functools.partial(step_kernel, cfg),
        out_shape=(jax.ShapeDtypeStruct(tables.shape, f32), jax.ShapeDtypeStruct(accumulator.shape, f32)),
        in_specs=[hbm] * 4,
        out_specs=(vmem, vmem),
        scratch_shapes=[
            *[pltpu.VMEM(replica_grads.shape[2:], replica_grads.dtype) for _ in range(ntab)],
            *[pltpu.VMEM((per, width, BLOCK), f32) for _ in range(ntab)],
            *[pltpu.VMEM((cols, n, BLOCK), f32) for _, _, n in pieces],
            pltpu.VMEM(block_ids.shape, i32),
            pltpu.VMEM((ntab, 2, nblk), i32),
            pltpu.VMEM((ntab, 1, wide), i32),
            pltpu.SMEM((ntab, 2, nblk), i32),
            pltpu.SMEM((ntab, 1, wide), i32),
            pltpu.VMEM((side - 1, side, slots, width, BLOCK), f32),
            pltpu.VMEM((side - 1, side - 1, slots, width, BLOCK), f32),
            pltpu.VMEM((side - 1, slots, width, BLOCK), f32),
            pltpu.VMEM((2 * side - 2, slots, width, BLOCK), f32),
            pltpu.VMEM((ntab, per, BLOCK), f32),
            pltpu.VMEM((ntab, per, BLOCK), f32),
            pltpu.VMEM((cols - 1, slots, BLOCK), f32),
            dma((3 + ntab,)), dma((2, ntab)), dma((3,)),
            dma((n_pieces,)), dma((n_pieces,)), dma((n_pieces,)),
            pltpu.SemaphoreType.REGULAR, pltpu.SemaphoreType.REGULAR,
        ],
        compiler_params=pltpu.CompilerParams(
            collective_id=0, has_side_effects=True, vmem_limit_bytes=32 * 2**20),
        name="exchange",
    )(*[pltpu.with_memory_space_constraint(a, pltpu.HBM) for a in (block_ids, replica_grads, tables, accumulator)])
    return pl.pallas_call(
        store_kernel,
        out_shape=(jax.ShapeDtypeStruct(tables.shape, f32), jax.ShapeDtypeStruct(accumulator.shape, f32)),
        in_specs=[vmem, vmem],
        out_specs=(hbm, hbm),
        scratch_shapes=[dma((ntab, width // 8)), dma(())],
        compiler_params=pltpu.CompilerParams(vmem_limit_bytes=2**20),
        name="store",
    )(image, new_acc)


def solution(mesh):
    return jax.shard_map(
        functools.partial(body, mesh),
        mesh=mesh,
        in_specs=(P(None, "col", "rep"), P(None, "rep"), P("rep", None, "col", None), P()),
        out_specs=(P(None, "col", "rep"), P(None, "rep")),
        check_vma=False,
    )
```

```python
import functools
import math

import jax
import jax.numpy as jnp
from jax import lax
from jax.experimental import pallas as pl
from jax.experimental.pallas import tpu as pltpu
from jax.sharding import PartitionSpec as P

BLOCK = 128
MESH = pl.DeviceIdType.MESH


def cuts(per, last):
    if per % 8:
        return [1] * per
    unit = per // 8
    tail = max(1, 3 * unit // 4)
    return [2 * unit] * 2 + [2 * unit - tail] * 2 + [tail] * 2 if last else [4 * unit] * 2


def layout(mesh, shape, n_slab):
    reps, cols = mesh.shape["rep"], mesh.shape["col"]
    inner = math.isqrt(reps)
    while reps % inner:
        inner -= 1
    ntab, width, local_rows = shape
    per = n_slab // BLOCK // reps
    pieces = []
    for t in range(ntab):
        start = 0
        for n in cuts(per, t == ntab - 1):
            pieces.append((t, start, n))
            start += n
    steered = 2 if inner == 2 and reps == 4 else 0
    return dict(steered=steered, reps=reps, cols=cols, inner=inner, outer=reps // inner, ntab=ntab, width=width,
                per=per, nblk=n_slab // BLOCK, local=local_rows // BLOCK, dim=width * cols, pieces=pieces)


def lanes(i):
    return pl.ds(i * BLOCK, BLOCK)


def step_kernel(cfg, ids_hbm, grads_hbm, tables_hbm, acc_hbm, image, new_acc, *scratch):
    reps, cols, inner, outer = cfg["reps"], cfg["cols"], cfg["inner"], cfg["outer"]
    ntab, width, per, nblk = cfg["ntab"], cfg["width"], cfg["per"], cfg["nblk"]
    local, dim, pieces = cfg["local"], cfg["dim"], cfg["pieces"]
    n_pieces = len(pieces)
    scratch = list(scratch)

    def take(n):
        out = scratch[:n]
        del scratch[:n]
        return out

    g, totals = take(ntab), take(ntab)
    sq = take(n_pieces)
    (ids_v, order_v, code_v, order_s, code_s, packed, landed, relayed, arrived, acc_slot, step, sent, spare,
     in_sem, meta_sem, send_sem, far_sem, own_sem, sq_sem, up, down, spare_sem) = scratch
    first_steered = n_pieces - cfg["steered"]

    me = lax.axis_index("rep")
    my_col = lax.axis_index("col")
    x, y = lax.rem(me, inner), me // inner

    ids_copy = pltpu.make_async_copy(ids_hbm, ids_v, in_sem.at[0])
    ids_copy.start()
    grad_copies = [pltpu.make_async_copy(grads_hbm.at[0, t], g[t], in_sem.at[3 + t]) for t in range(ntab)]
    for copy in grad_copies:
        copy.start()

    barrier = pltpu.get_barrier_semaphore()
    for f in range(1, inner):
        pl.semaphore_signal(barrier, inc=1, device_id={"rep": y * inner + lax.rem(x + f, inner)}, device_id_type=MESH)
    for f in range(1, outer):
        pl.semaphore_signal(barrier, inc=1, device_id={"rep": lax.rem(y + f, outer) * inner + x}, device_id_type=MESH)

    def pass_on(sem, way):
        pl.semaphore_signal(sem, inc=1, device_id={"col": my_col + way}, device_id_type=MESH)

    pl.when(my_col > 0)(lambda: pass_on(barrier, -1))
    pl.when(my_col < cols - 1)(lambda: pass_on(barrier, 1))

    acc_copy = pltpu.make_async_copy(acc_hbm, new_acc, in_sem.at[1])
    acc_copy.start()
    table_copy = pltpu.make_async_copy(tables_hbm, image, in_sem.at[2])
    table_copy.start()

    lane = lax.broadcasted_iota(jnp.int32, (nblk, nblk), 1)
    slot = lax.broadcasted_iota(jnp.int32, (nblk, nblk), 0)
    wide = code_v.shape[2]
    own_block = lax.broadcasted_iota(jnp.int32, (nblk, wide), 1) + me * local

    def order_copy(t):
        return pltpu.make_async_copy(order_v.at[t], order_s.at[t], meta_sem.at[0, t])

    def code_copy(t):
        return pltpu.make_async_copy(code_v.at[t], code_s.at[t], meta_sem.at[1, t])

    def rank_blocks(t):
        across = jnp.broadcast_to(ids_v[pl.ds(t, 1), :], (nblk, nblk))
        down = across.T
        place = jnp.sum(jnp.where(down < across, 1, 0), axis=0, keepdims=True)
        hit = jnp.broadcast_to(place, (nblk, nblk)).T == lane
        order = jnp.sum(jnp.where(hit, slot, 0), axis=0, keepdims=True)
        block = jnp.sum(jnp.where(hit, down, 0), axis=0, keepdims=True) - me * local
        order_v[t, pl.ds(0, 1), :] = jnp.clip(order, 0, nblk - 1)
        order_v[t, pl.ds(1, 1), :] = jnp.clip(block, 0, local - 1)
        order_copy(t).start()
        col = jnp.broadcast_to(down[:, :1], (nblk, wide))
        below = jnp.sum(jnp.where(col < own_block, 1, 0), axis=0, keepdims=True) - me * per
        found = jnp.sum(jnp.where(col == own_block, 1, 0), axis=0, keepdims=True)
        code_v[t, pl.ds(0, 1), :] = jnp.where(found > 0, jnp.clip(below, 0, per - 1), -1)
        code_copy(t).start()

    ids_copy.wait()
    rank_blocks(0)

    def axes(p):
        return (inner, outer) if p % 2 == 0 else (outer, inner)

    def rank(p, f, s):
        if p % 2 == 0:
            return lax.rem(y + s, outer) * inner + lax.rem(x + f, inner)
        return lax.rem(y + f, outer) * inner + lax.rem(x + s, inner)

    def span(p):
        t, start, n = pieces[p]
        return pl.ds(t * per + start, n)

    def mine(t, owner, i):
        at = order_s[t, 0, owner * per + i]
        return g[t][:, lanes(at)].astype(jnp.float32)

    def first_copy(p, f, s):
        here = arrived.at[f - 1, span(p)] if s == 0 else landed.at[f - 1, s - 1, span(p)]
        return pltpu.make_async_remote_copy(
            packed.at[f - 1, s, span(p)], here, send_sem.at[0], own_sem.at[p] if s == 0 else far_sem.at[p],
            device_id={"rep": rank(p, f, 0)}, device_id_type=MESH)

    def second_copy(p, s):
        nf = axes(p)[0]
        return pltpu.make_async_remote_copy(
            relayed.at[s - 1, span(p)], arrived.at[nf - 2 + s, span(p)], send_sem.at[1], own_sem.at[p],
            device_id={"rep": rank(p, 0, s)}, device_id_type=MESH)

    def square_copy(p, f):
        return pltpu.make_async_remote_copy(
            sq[p].at[my_col], sq[p].at[my_col], send_sem.at[2], sq_sem.at[p],
            device_id={"col": lax.rem(my_col + f, cols)}, device_id_type=MESH)

    def wait_all(ref, sem):
        pltpu.make_async_copy(ref, ref, sem).wait()

    def pack(p, f, s):
        t, start, n = pieces[p]
        owner = rank(p, f, s)
        for i in range(n):
            packed[f - 1, s, t * per + start + i] = mine(t, owner, start + i)
        first_copy(p, f, s).start()

    beside_me = (y * inner + lax.rem(x + 1, inner), lax.rem(y + 1, outer) * inner + x)
    across_me = lax.rem(y + 1, outer) * inner + lax.rem(x + 1, inner)

    def way(p, owner):
        return jnp.where(owner == 1, 0, jnp.where(owner == inner, 1, p % 2))

    def steered_far(p):
        t, start, n = pieces[p]
        first = way(p, across_me)
        for i in range(n):
            packed[0, 1, t * per + start + i] = mine(t, across_me, start + i)
        b = p - first_steered
        pltpu.make_async_remote_copy(
            packed.at[0, 1, span(p)], spare.at[first, b], send_sem.at[0], spare_sem.at[first, b],
            device_id={"rep": jnp.where(first == 0, beside_me[0], beside_me[1])}, device_id_type=MESH).start()

    def steered_send(p, d, relaying):
        t, start, n = pieces[p]
        owner, b = beside_me[d], p - first_steered
        out = packed.at[0, 0] if d == 0 else relayed.at[0]

        def send():
            if relaying:
                wait_all(spare.at[1 - d, b], spare_sem.at[1 - d, b])
            for i in range(n):
                acc = mine(t, owner, start + i)
                if relaying:
                    acc = acc + spare[1 - d, b, i]
                out[t * per + start + i] = acc
            pltpu.make_async_remote_copy(
                out.at[span(p)], arrived.at[d, span(p)], send_sem.at[d], own_sem.at[p],
                device_id={"rep": owner}, device_id_type=MESH).start()

        pl.when((way(p, owner) != d) if relaying else (way(p, owner) == d))(send)

    def send_far(p):
        if p >= first_steered:
            steered_far(p)
            return
        nf, ns = axes(p)
        for s in range(1, ns):
            for f in range(1, nf):
                pack(p, f, s)

    def send_near(p):
        if p >= first_steered:
            for d in range(2):
                steered_send(p, d, False)
            return
        for f in range(1, axes(p)[0]):
            pack(p, f, 0)

    def relay(p):
        if p >= first_steered:
            for d in range(2):
                steered_send(p, d, True)
            return
        t, start, n = pieces[p]
        nf, ns = axes(p)
        wait_all(landed.at[pl.ds(0, nf - 1), pl.ds(0, ns - 1), span(p)], far_sem.at[p])
        for s in range(1, ns):
            owner = rank(p, 0, s)
            for i in range(n):
                acc = mine(t, owner, start + i)
                for f in range(1, nf):
                    acc = acc + landed[f - 1, s - 1, t * per + start + i]
                relayed[s - 1, t * per + start + i] = acc
            second_copy(p, s).start()

    def finish(p):
        t, start, n = pieces[p]
        nf, ns = axes(p)
        wait_all(arrived.at[pl.ds(0, nf + ns - 2), span(p)], own_sem.at[p])
        for i in range(n):
            acc = mine(t, me, start + i)
            for k in range(nf + ns - 2):
                acc = acc + arrived[k, t * per + start + i]
            totals[t][start + i] = acc
            sq[p][my_col, pl.ds(i, 1), :] = jnp.sum(acc * acc, axis=0, keepdims=True)
        for f in range(1, cols):
            square_copy(p, f).start()

    def gather(p):
        t, start, n = pieces[p]
        wait_all(sq[p].at[pl.ds(0, cols - 1)], sq_sem.at[p])
        acc = sq[p][0]
        for f in range(1, cols):
            acc = acc + sq[p][f]
        fresh = acc_slot[t, pl.ds(start, n), :] + acc * (1.0 / dim)
        acc_slot[t, pl.ds(start, n), :] = fresh
        step[t, pl.ds(start, n), :] = 0.1 / (jnp.sqrt(fresh) + 1e-8)
        for i in range(start, start + n):
            totals[t][i] = totals[t][i] * step[t, pl.ds(i, 1), :]

    def place(t):
        for b in range(local):
            code = code_s[t, 0, b]
            at = jnp.maximum(code, 0)
            where = pl.ds(b * BLOCK, BLOCK)
            hit = jnp.full((width, BLOCK), code, jnp.int32) >= 0
            old = image[t, :, where]
            image[t, :, where] = jnp.where(hit, old - totals[t][at], old)
            old_acc = new_acc[pl.ds(t, 1), where]
            new_acc[pl.ds(t, 1), where] = jnp.where(hit[:1], acc_slot[t, pl.ds(at, 1), :], old_acc)

    def sweep(sem, way, behind, ahead):
        pl.when(behind)(lambda: pl.semaphore_wait(sem, 1))
        pl.when(ahead)(lambda: pass_on(sem, way))

    for t in range(ntab):
        order_copy(t).wait()
        grad_copies[t].wait()
        if t == 0:
            beside = jnp.minimum(my_col, 1) + jnp.minimum(cols - 1 - my_col, 1)
            pl.semaphore_wait(barrier, inner - 1 + outer - 1 + beside)
        for p in range(n_pieces):
            if pieces[p][0] == t:
                send_far(p)
        if t + 1 < ntab:
            rank_blocks(t + 1)
    for p in range(n_pieces):
        send_near(p)

    acc_copy.wait()
    for t in range(ntab):
        for i in range(per):
            block = order_s[t, 1, me * per + i]
            acc_slot[t, pl.ds(i, 1), :] = new_acc[pl.ds(t, 1), lanes(block)]

    for p in range(n_pieces):
        relay(p)
    sweep(up, 1, my_col > 0, my_col < cols - 1)
    sweep(down, -1, my_col < cols - 1, my_col > 0)
    table_copy.wait()
    for t in range(ntab):
        code_copy(t).wait()
    for p in range(n_pieces):
        finish(p)
    for p in range(n_pieces):
        gather(p)
        t = pieces[p][0]
        if p + 1 == n_pieces or pieces[p + 1][0] != t:
            place(t)

    if inner == outer:
        wait_all(packed, send_sem.at[0])
        wait_all(relayed, send_sem.at[1])
    else:
        for p in range(n_pieces):
            nf, ns = axes(p)
            wait_all(packed.at[pl.ds(0, nf - 1), pl.ds(0, ns), span(p)], send_sem.at[0])
            wait_all(relayed.at[pl.ds(0, ns - 1), span(p)], send_sem.at[1])
    wait_all(sent, send_sem.at[2])


def store_kernel(image, acc, tables_out, acc_out, sem, acc_sem):
    copies = [pltpu.make_async_copy(acc, acc_out, acc_sem)]
    for t in range(image.shape[0]):
        copies.append(pltpu.make_async_copy(image.at[t], tables_out.at[t], sem.at[t]))
    for copy in copies:
        copy.start()
    for copy in copies:
        copy.wait()


def body(mesh, tables, accumulator, replica_grads, block_ids):
    cfg = layout(mesh, tables.shape, replica_grads.shape[3])
    ntab, width, per, nblk = cfg["ntab"], cfg["width"], cfg["per"], cfg["nblk"]
    cols, pieces = cfg["cols"], cfg["pieces"]
    side = max(cfg["inner"], cfg["outer"])
    slots, n_pieces = ntab * per, len(pieces)
    wide = -(-cfg["local"] // BLOCK) * BLOCK
    f32, i32 = jnp.float32, jnp.int32
    dma = pltpu.SemaphoreType.DMA
    hbm = pl.BlockSpec(memory_space=pltpu.HBM)
    vmem = pl.BlockSpec(memory_space=pltpu.VMEM)
    image, new_acc = pl.pallas_call(
        functools.partial(step_kernel, cfg),
        out_shape=(jax.ShapeDtypeStruct(tables.shape, f32), jax.ShapeDtypeStruct(accumulator.shape, f32)),
        in_specs=[hbm] * 4,
        out_specs=(vmem, vmem),
        scratch_shapes=[
            *[pltpu.VMEM(replica_grads.shape[2:], replica_grads.dtype) for _ in range(ntab)],
            *[pltpu.VMEM((per, width, BLOCK), f32) for _ in range(ntab)],
            *[pltpu.VMEM((cols, n, BLOCK), f32) for _, _, n in pieces],
            pltpu.VMEM(block_ids.shape, i32),
            pltpu.VMEM((ntab, 2, nblk), i32),
            pltpu.VMEM((ntab, 1, wide), i32),
            pltpu.SMEM((ntab, 2, nblk), i32),
            pltpu.SMEM((ntab, 1, wide), i32),
            pltpu.VMEM((side - 1, side, slots, width, BLOCK), f32),
            pltpu.VMEM((side - 1, side - 1, slots, width, BLOCK), f32),
            pltpu.VMEM((side - 1, slots, width, BLOCK), f32),
            pltpu.VMEM((2 * side - 2, slots, width, BLOCK), f32),
            pltpu.VMEM((ntab, per, BLOCK), f32),
            pltpu.VMEM((ntab, per, BLOCK), f32),
            pltpu.VMEM((cols - 1, slots, BLOCK), f32),
            pltpu.VMEM((2, 2, pieces[-1][2], width, BLOCK), f32),
            dma((3 + ntab,)), dma((2, ntab)), dma((3,)),
            dma((n_pieces,)), dma((n_pieces,)), dma((n_pieces,)),
            pltpu.SemaphoreType.REGULAR, pltpu.SemaphoreType.REGULAR, dma((2, 2)),
        ],
        compiler_params=pltpu.CompilerParams(
            collective_id=0, has_side_effects=True, vmem_limit_bytes=32 * 2**20),
        name="exchange",
    )(*[pltpu.with_memory_space_constraint(a, pltpu.HBM) for a in (block_ids, replica_grads, tables, accumulator)])
    return pl.pallas_call(
        store_kernel,
        out_shape=(jax.ShapeDtypeStruct(tables.shape, f32), jax.ShapeDtypeStruct(accumulator.shape, f32)),
        in_specs=[vmem, vmem],
        out_specs=(hbm, hbm),
        scratch_shapes=[dma((ntab,)), dma(())],
        compiler_params=pltpu.CompilerParams(vmem_limit_bytes=2**20),
        name="store",
    )(image, new_acc)


def solution(mesh):
    return jax.shard_map(
        functools.partial(body, mesh),
        mesh=mesh,
        in_specs=(P(None, "col", "rep"), P(None, "rep"), P("rep", None, "col", None), P()),
        out_specs=(P(None, "col", "rep"), P(None, "rep")),
        check_vma=False,
    )
```

```python
import functools
import math

import jax
import jax.numpy as jnp
from jax import lax
from jax.experimental import pallas as pl
from jax.experimental.pallas import tpu as pltpu
from jax.sharding import PartitionSpec as P

BLOCK = 128
MESH = pl.DeviceIdType.MESH


def cuts(per, last):
    if per % 8:
        return [1] * per
    unit = per // 8
    tail = max(1, 3 * unit // 4)
    return [2 * unit] * 2 + [2 * unit - tail] * 2 + [tail] * 2 if last else [unit] * 2 + [3 * unit] * 2


def layout(mesh, shape, n_slab):
    reps, cols = mesh.shape["rep"], mesh.shape["col"]
    inner = math.isqrt(reps)
    while reps % inner:
        inner -= 1
    ntab, width, local_rows = shape
    per = n_slab // BLOCK // reps
    pieces = []
    for t in range(ntab):
        start = 0
        for n in cuts(per, t == ntab - 1):
            pieces.append((t, start, n))
            start += n
    steered = 2 if inner == 2 and reps == 4 else 0
    return dict(steered=steered, reps=reps, cols=cols, inner=inner, outer=reps // inner, ntab=ntab, width=width,
                per=per, nblk=n_slab // BLOCK, local=local_rows // BLOCK, dim=width * cols, pieces=pieces)


def lanes(i):
    return pl.ds(i * BLOCK, BLOCK)


def step_kernel(cfg, ids_hbm, grads_hbm, tables_hbm, acc_hbm, image, new_acc, *scratch):
    reps, cols, inner, outer = cfg["reps"], cfg["cols"], cfg["inner"], cfg["outer"]
    ntab, width, per, nblk = cfg["ntab"], cfg["width"], cfg["per"], cfg["nblk"]
    local, dim, pieces = cfg["local"], cfg["dim"], cfg["pieces"]
    n_pieces = len(pieces)
    scratch = list(scratch)

    def take(n):
        out = scratch[:n]
        del scratch[:n]
        return out

    g = [take(2) for _ in range(ntab)]
    totals = take(ntab)
    half = width // 2
    sq = take(n_pieces)
    (ids_v, order_v, code_v, order_s, code_s, packed, landed, relayed, arrived, acc_slot, step, sent, spare,
     in_sem, meta_sem, send_sem, far_sem, own_sem, sq_sem, up, down, spare_sem) = scratch
    first_steered = n_pieces - cfg["steered"]

    me = lax.axis_index("rep")
    my_col = lax.axis_index("col")
    x, y = lax.rem(me, inner), me // inner

    ids_copy = pltpu.make_async_copy(ids_hbm, ids_v, in_sem.at[0])
    ids_copy.start()
    grad_copies = [[pltpu.make_async_copy(grads_hbm.at[0, t, pl.ds(h * half, half)], g[t][h], in_sem.at[3 + 2 * t + h])
                    for h in range(2)] for t in range(ntab)]
    for copy in grad_copies[0]:
        copy.start()

    barrier = pltpu.get_barrier_semaphore()
    for f in range(1, inner):
        pl.semaphore_signal(barrier, inc=1, device_id={"rep": y * inner + lax.rem(x + f, inner)}, device_id_type=MESH)
    for f in range(1, outer):
        pl.semaphore_signal(barrier, inc=1, device_id={"rep": lax.rem(y + f, outer) * inner + x}, device_id_type=MESH)

    def pass_on(sem, way):
        pl.semaphore_signal(sem, inc=1, device_id={"col": my_col + way}, device_id_type=MESH)

    pl.when(my_col > 0)(lambda: pass_on(barrier, -1))
    pl.when(my_col < cols - 1)(lambda: pass_on(barrier, 1))

    acc_copy = pltpu.make_async_copy(acc_hbm, new_acc, in_sem.at[1])
    table_copy = pltpu.make_async_copy(tables_hbm, image, in_sem.at[2])

    lane = lax.broadcasted_iota(jnp.int32, (nblk, nblk), 1)
    slot = lax.broadcasted_iota(jnp.int32, (nblk, nblk), 0)
    wide = code_v.shape[2]
    own_block = lax.broadcasted_iota(jnp.int32, (nblk, wide), 1) + me * local

    def order_copy(t):
        return pltpu.make_async_copy(order_v.at[t], order_s.at[t], meta_sem.at[0, t])

    def code_copy(t):
        return pltpu.make_async_copy(code_v.at[t], code_s.at[t], meta_sem.at[1, t])

    def rank_blocks(t):
        across = jnp.broadcast_to(ids_v[pl.ds(t, 1), :], (nblk, nblk))
        column = across.T
        place = jnp.sum(jnp.where(column < across, 1, 0), axis=0, keepdims=True)
        hit = jnp.broadcast_to(place, (nblk, nblk)).T == lane
        order = jnp.sum(jnp.where(hit, slot, 0), axis=0, keepdims=True)
        block = jnp.sum(jnp.where(hit, column, 0), axis=0, keepdims=True) - me * local
        order = jnp.clip(order, 0, nblk - 1)
        order_v[t, pl.ds(0, 1), :] = order
        order_v[t, pl.ds(1, 1), :] = jnp.clip(block, 0, local - 1)
        order_copy(t).start()
        return order, column

    def rank_local(t, column):
        col = jnp.broadcast_to(column[:, :1], (nblk, wide))
        below = jnp.sum(jnp.where(col < own_block, 1, 0), axis=0, keepdims=True) - me * per
        found = jnp.sum(jnp.where(col == own_block, 1, 0), axis=0, keepdims=True)
        code_v[t, pl.ds(0, 1), :] = jnp.where(found > 0, jnp.clip(below, 0, per - 1), -1)
        code_copy(t).start()

    ids_copy.wait()
    first_order, column = rank_blocks(0)

    def axes(p):
        return (inner, outer) if p % 2 == 0 else (outer, inner)

    def rank(p, f, s):
        if p % 2 == 0:
            return lax.rem(y + s, outer) * inner + lax.rem(x + f, inner)
        return lax.rem(y + f, outer) * inner + lax.rem(x + s, inner)

    def span(p):
        t, start, n = pieces[p]
        return pl.ds(t * per + start, n)

    def mine(t, owner, i):
        where = lanes(order_s[t, 0, owner * per + i])
        return jnp.concatenate([part[:, where].astype(jnp.float32) for part in g[t]], axis=0)

    def first_copy(p, f, s):
        here = arrived.at[f - 1, span(p)] if s == 0 else landed.at[f - 1, s - 1, span(p)]
        return pltpu.make_async_remote_copy(
            packed.at[f - 1, s, span(p)], here, send_sem.at[0], own_sem.at[p] if s == 0 else far_sem.at[p],
            device_id={"rep": rank(p, f, 0)}, device_id_type=MESH)

    def second_copy(p, s):
        nf = axes(p)[0]
        return pltpu.make_async_remote_copy(
            relayed.at[s - 1, span(p)], arrived.at[nf - 2 + s, span(p)], send_sem.at[1], own_sem.at[p],
            device_id={"rep": rank(p, 0, s)}, device_id_type=MESH)

    def square_copy(p, f):
        return pltpu.make_async_remote_copy(
            sq[p].at[my_col], sq[p].at[my_col], send_sem.at[2], sq_sem.at[p],
            device_id={"col": lax.rem(my_col + f, cols)}, device_id_type=MESH)

    def wait_all(ref, sem):
        pltpu.make_async_copy(ref, ref, sem).wait()

    def pack(p, f, s):
        t, start, n = pieces[p]
        owner = rank(p, f, s)
        for i in range(n):
            packed[f - 1, s, t * per + start + i] = mine(t, owner, start + i)
        first_copy(p, f, s).start()

    beside_me = (y * inner + lax.rem(x + 1, inner), lax.rem(y + 1, outer) * inner + x)
    across_me = lax.rem(y + 1, outer) * inner + lax.rem(x + 1, inner)

    def way(p, owner):
        return jnp.where(owner == 1, 0, jnp.where(owner == inner, 1, p % 2))

    def steered_far(p):
        t, start, n = pieces[p]
        first = way(p, across_me)
        for i in range(n):
            packed[0, 1, t * per + start + i] = mine(t, across_me, start + i)
        b = p - first_steered
        pltpu.make_async_remote_copy(
            packed.at[0, 1, span(p)], spare.at[first, b], send_sem.at[0], spare_sem.at[first, b],
            device_id={"rep": jnp.where(first == 0, beside_me[0], beside_me[1])}, device_id_type=MESH).start()

    def steered_send(p, d, relaying):
        t, start, n = pieces[p]
        owner, b = beside_me[d], p - first_steered
        out = packed.at[0, 0] if d == 0 else relayed.at[0]

        def send():
            if relaying:
                wait_all(spare.at[1 - d, b], spare_sem.at[1 - d, b])
            for i in range(n):
                acc = mine(t, owner, start + i)
                if relaying:
                    acc = acc + spare[1 - d, b, i]
                out[t * per + start + i] = acc
            pltpu.make_async_remote_copy(
                out.at[span(p)], arrived.at[d, span(p)], send_sem.at[d], own_sem.at[p],
                device_id={"rep": owner}, device_id_type=MESH).start()

        pl.when((way(p, owner) != d) if relaying else (way(p, owner) == d))(send)

    def first_far(p, picked, h):
        t, start, n = pieces[p]
        nf, ns = axes(p)
        dims = pl.ds(h * half, half)
        for s in range(1, ns):
            for f in range(1, nf):
                for i in range(n):
                    block = g[t][h][:, lanes(picked[f, s][i])].astype(jnp.float32)
                    packed[f - 1, s, t * per + start + i, dims] = block
                pltpu.make_async_remote_copy(
                    packed.at[f - 1, s, span(p), dims], landed.at[f - 1, s - 1, span(p), dims],
                    send_sem.at[0], far_sem.at[p], device_id={"rep": rank(p, f, 0)}, device_id_type=MESH).start()

    def pick(p):
        _, start, n = pieces[p]
        nf, ns = axes(p)
        picked = {}
        for s in range(1, ns):
            for f in range(1, nf):
                row = pltpu.roll(first_order, lax.rem(nblk - rank(p, f, s) * per, nblk), 1)
                picked[f, s] = [row[0, start + i] for i in range(n)]
        return picked

    def send_far(p):
        if p >= first_steered:
            steered_far(p)
            return
        nf, ns = axes(p)
        for s in range(1, ns):
            for f in range(1, nf):
                pack(p, f, s)

    def send_near(p):
        if p >= first_steered:
            for d in range(2):
                steered_send(p, d, False)
            return
        for f in range(1, axes(p)[0]):
            pack(p, f, 0)

    def relay(p):
        if p >= first_steered:
            for d in range(2):
                steered_send(p, d, True)
            return
        t, start, n = pieces[p]
        nf, ns = axes(p)
        wait_all(landed.at[pl.ds(0, nf - 1), pl.ds(0, ns - 1), span(p)], far_sem.at[p])
        for s in range(1, ns):
            owner = rank(p, 0, s)
            for i in range(n):
                acc = mine(t, owner, start + i)
                for f in range(1, nf):
                    acc = acc + landed[f - 1, s - 1, t * per + start + i]
                relayed[s - 1, t * per + start + i] = acc
            second_copy(p, s).start()

    def finish(p):
        t, start, n = pieces[p]
        nf, ns = axes(p)
        wait_all(arrived.at[pl.ds(0, nf + ns - 2), span(p)], own_sem.at[p])
        for i in range(n):
            acc = mine(t, me, start + i)
            for k in range(nf + ns - 2):
                acc = acc + arrived[k, t * per + start + i]
            totals[t][start + i] = acc
            sq[p][my_col, pl.ds(i, 1), :] = jnp.sum(acc * acc, axis=0, keepdims=True)
        for f in range(1, cols):
            square_copy(p, f).start()

    def gather(p):
        t, start, n = pieces[p]
        wait_all(sq[p].at[pl.ds(0, cols - 1)], sq_sem.at[p])
        acc = sq[p][0]
        for f in range(1, cols):
            acc = acc + sq[p][f]
        fresh = acc_slot[t, pl.ds(start, n), :] + acc * (1.0 / dim)
        acc_slot[t, pl.ds(start, n), :] = fresh
        step[t, pl.ds(start, n), :] = 0.1 / (jnp.sqrt(fresh) + 1e-8)
        for i in range(start, start + n):
            totals[t][i] = totals[t][i] * step[t, pl.ds(i, 1), :]

    def place(t):
        for b in range(local):
            code = code_s[t, 0, b]
            at = jnp.maximum(code, 0)
            where = pl.ds(b * BLOCK, BLOCK)
            hit = jnp.full((width, BLOCK), code, jnp.int32) >= 0
            old = image[t, :, where]
            image[t, :, where] = jnp.where(hit, old - totals[t][at], old)
            old_acc = new_acc[pl.ds(t, 1), where]
            new_acc[pl.ds(t, 1), where] = jnp.where(hit[:1], acc_slot[t, pl.ds(at, 1), :], old_acc)

    def sweep(sem, way, behind, ahead):
        pl.when(behind)(lambda: pl.semaphore_wait(sem, 1))
        pl.when(ahead)(lambda: pass_on(sem, way))

    picked = [pick(p) for p in range(2)]
    beside = jnp.minimum(my_col, 1) + jnp.minimum(cols - 1 - my_col, 1)
    pl.semaphore_wait(barrier, inner - 1 + outer - 1 + beside)
    for h in range(2):
        grad_copies[0][h].wait()
        for p in range(2):
            first_far(p, picked[p], h)
    for copy in [*sum(grad_copies[1:], []), acc_copy, table_copy]:
        copy.start()
    for t in range(ntab):
        if t > 0:
            for copy in grad_copies[t]:
                copy.wait()
        order_copy(t).wait()
        for p in range(2, n_pieces):
            if pieces[p][0] == t:
                send_far(p)
        rank_local(t, column)
        if t + 1 < ntab:
            column = rank_blocks(t + 1)[1]
    for p in range(n_pieces):
        send_near(p)

    acc_copy.wait()
    for t in range(ntab):
        for i in range(per):
            block = order_s[t, 1, me * per + i]
            acc_slot[t, pl.ds(i, 1), :] = new_acc[pl.ds(t, 1), lanes(block)]

    for p in range(n_pieces):
        relay(p)
    sweep(up, 1, my_col > 0, my_col < cols - 1)
    sweep(down, -1, my_col < cols - 1, my_col > 0)
    table_copy.wait()
    for t in range(ntab):
        code_copy(t).wait()
    for p in range(n_pieces):
        finish(p)
    for p in range(n_pieces):
        gather(p)
        t = pieces[p][0]
        if p + 1 == n_pieces or pieces[p + 1][0] != t:
            place(t)

    if inner == outer:
        wait_all(packed, send_sem.at[0])
        wait_all(relayed, send_sem.at[1])
    else:
        for p in range(n_pieces):
            nf, ns = axes(p)
            wait_all(packed.at[pl.ds(0, nf - 1), pl.ds(0, ns), span(p)], send_sem.at[0])
            wait_all(relayed.at[pl.ds(0, ns - 1), span(p)], send_sem.at[1])
    wait_all(sent, send_sem.at[2])


def store_kernel(image, acc, tables_out, acc_out, sem, acc_sem):
    copies = [pltpu.make_async_copy(acc, acc_out, acc_sem)]
    for t in range(image.shape[0]):
        copies.append(pltpu.make_async_copy(image.at[t], tables_out.at[t], sem.at[t]))
    for copy in copies:
        copy.start()
    for copy in copies:
        copy.wait()


def body(mesh, tables, accumulator, replica_grads, block_ids):
    cfg = layout(mesh, tables.shape, replica_grads.shape[3])
    ntab, width, per, nblk = cfg["ntab"], cfg["width"], cfg["per"], cfg["nblk"]
    cols, pieces = cfg["cols"], cfg["pieces"]
    side = max(cfg["inner"], cfg["outer"])
    slots, n_pieces = ntab * per, len(pieces)
    wide = -(-cfg["local"] // BLOCK) * BLOCK
    f32, i32 = jnp.float32, jnp.int32
    dma = pltpu.SemaphoreType.DMA
    hbm = pl.BlockSpec(memory_space=pltpu.HBM)
    vmem = pl.BlockSpec(memory_space=pltpu.VMEM)
    image, new_acc = pl.pallas_call(
        functools.partial(step_kernel, cfg),
        out_shape=(jax.ShapeDtypeStruct(tables.shape, f32), jax.ShapeDtypeStruct(accumulator.shape, f32)),
        in_specs=[hbm] * 4,
        out_specs=(vmem, vmem),
        scratch_shapes=[
            *[pltpu.VMEM((width // 2, replica_grads.shape[3]), replica_grads.dtype) for _ in range(2 * ntab)],
            *[pltpu.VMEM((per, width, BLOCK), f32) for _ in range(ntab)],
            *[pltpu.VMEM((cols, n, BLOCK), f32) for _, _, n in pieces],
            pltpu.VMEM(block_ids.shape, i32),
            pltpu.VMEM((ntab, 2, nblk), i32),
            pltpu.VMEM((ntab, 1, wide), i32),
            pltpu.SMEM((ntab, 2, nblk), i32),
            pltpu.SMEM((ntab, 1, wide), i32),
            pltpu.VMEM((side - 1, side, slots, width, BLOCK), f32),
            pltpu.VMEM((side - 1, side - 1, slots, width, BLOCK), f32),
            pltpu.VMEM((side - 1, slots, width, BLOCK), f32),
            pltpu.VMEM((2 * side - 2, slots, width, BLOCK), f32),
            pltpu.VMEM((ntab, per, BLOCK), f32),
            pltpu.VMEM((ntab, per, BLOCK), f32),
            pltpu.VMEM((cols - 1, slots, BLOCK), f32),
            pltpu.VMEM((2, 2, pieces[-1][2], width, BLOCK), f32),
            dma((3 + 2 * ntab,)), dma((2, ntab)), dma((3,)),
            dma((n_pieces,)), dma((n_pieces,)), dma((n_pieces,)),
            pltpu.SemaphoreType.REGULAR, pltpu.SemaphoreType.REGULAR, dma((2, 2)),
        ],
        compiler_params=pltpu.CompilerParams(
            collective_id=0, has_side_effects=True, vmem_limit_bytes=32 * 2**20),
        name="exchange",
    )(*[pltpu.with_memory_space_constraint(a, pltpu.HBM) for a in (block_ids, replica_grads, tables, accumulator)])
    return pl.pallas_call(
        store_kernel,
        out_shape=(jax.ShapeDtypeStruct(tables.shape, f32), jax.ShapeDtypeStruct(accumulator.shape, f32)),
        in_specs=[vmem, vmem],
        out_specs=(hbm, hbm),
        scratch_shapes=[dma((ntab,)), dma(())],
        compiler_params=pltpu.CompilerParams(vmem_limit_bytes=2**20),
        name="store",
    )(image, new_acc)


def solution(mesh):
    return jax.shard_map(
        functools.partial(body, mesh),
        mesh=mesh,
        in_specs=(P(None, "col", "rep"), P(None, "rep"), P("rep", None, "col", None), P()),
        out_specs=(P(None, "col", "rep"), P(None, "rep")),
        check_vma=False,
    )
```

```python
import functools
import math

import jax
import jax.numpy as jnp
from jax import lax
from jax.experimental import pallas as pl
from jax.experimental.pallas import tpu as pltpu
from jax.sharding import PartitionSpec as P

BLOCK = 128
MESH = pl.DeviceIdType.MESH


def cuts(per, last):
    if per % 8:
        return [1] * per
    unit = per // 8
    tail = max(1, 3 * unit // 4)
    return [2 * unit] * 2 + [2 * unit - tail] * 2 + [tail] * 2 if last else [unit] * 2 + [3 * unit] * 2


def layout(mesh, shape, n_slab):
    reps, cols = mesh.shape["rep"], mesh.shape["col"]
    inner = math.isqrt(reps)
    while reps % inner:
        inner -= 1
    ntab, width, local_rows = shape
    per = n_slab // BLOCK // reps
    pieces = []
    for t in range(ntab):
        start = 0
        for n in cuts(per, t == ntab - 1):
            pieces.append((t, start, n))
            start += n
    steered = 2 if inner == 2 and reps == 4 else 0
    return dict(steered=steered, reps=reps, cols=cols, inner=inner, outer=reps // inner, ntab=ntab, width=width,
                per=per, nblk=n_slab // BLOCK, local=local_rows // BLOCK, dim=width * cols, pieces=pieces)


def lanes(i):
    return pl.ds(i * BLOCK, BLOCK)


def step_kernel(cfg, ids_hbm, grads_hbm, tables_hbm, acc_hbm, image, new_acc, *scratch):
    reps, cols, inner, outer = cfg["reps"], cfg["cols"], cfg["inner"], cfg["outer"]
    ntab, width, per, nblk = cfg["ntab"], cfg["width"], cfg["per"], cfg["nblk"]
    local, dim, pieces = cfg["local"], cfg["dim"], cfg["pieces"]
    n_pieces = len(pieces)
    scratch = list(scratch)

    def take(n):
        out = scratch[:n]
        del scratch[:n]
        return out

    g = [take(2) for _ in range(ntab)]
    totals = take(ntab)
    half = width // 2
    sq = take(n_pieces)
    (ids_v, order_v, code_v, order_s, code_s, packed, landed, relayed, arrived, acc_slot, step, sent, spare,
     in_sem, meta_sem, send_sem, far_sem, own_sem, sq_sem, up, down, spare_sem) = scratch
    first_steered = n_pieces - cfg["steered"]

    me = lax.axis_index("rep")
    my_col = lax.axis_index("col")
    x, y = lax.rem(me, inner), me // inner

    ids_copy = pltpu.make_async_copy(ids_hbm, ids_v, in_sem.at[0])
    ids_copy.start()
    grad_copies = [[pltpu.make_async_copy(grads_hbm.at[0, t, pl.ds(h * half, half)], g[t][h], in_sem.at[3 + 2 * t + h])
                    for h in range(2)] for t in range(ntab)]
    for copy in grad_copies[0]:
        copy.start()

    barrier = pltpu.get_barrier_semaphore()
    for f in range(1, inner):
        pl.semaphore_signal(barrier, inc=1, device_id={"rep": y * inner + lax.rem(x + f, inner)}, device_id_type=MESH)
    for f in range(1, outer):
        pl.semaphore_signal(barrier, inc=1, device_id={"rep": lax.rem(y + f, outer) * inner + x}, device_id_type=MESH)

    def pass_on(sem, way):
        pl.semaphore_signal(sem, inc=1, device_id={"col": my_col + way}, device_id_type=MESH)

    pl.when(my_col > 0)(lambda: pass_on(barrier, -1))
    pl.when(my_col < cols - 1)(lambda: pass_on(barrier, 1))

    acc_copy = pltpu.make_async_copy(acc_hbm, new_acc, in_sem.at[1])
    table_copy = pltpu.make_async_copy(tables_hbm, image, in_sem.at[2])

    lane = lax.broadcasted_iota(jnp.int32, (nblk, nblk), 1)
    slot = lax.broadcasted_iota(jnp.int32, (nblk, nblk), 0)
    wide = code_v.shape[2]
    own_block = lax.broadcasted_iota(jnp.int32, (nblk, wide), 1) + me * local

    def order_copy(t):
        return pltpu.make_async_copy(order_v.at[t], order_s.at[t], meta_sem.at[t])

    def code_copy(t):
        return pltpu.make_async_copy(code_v.at[t], code_s.at[t], meta_sem.at[ntab])

    def rank_blocks(t):
        across = jnp.broadcast_to(ids_v[pl.ds(t, 1), :], (nblk, nblk))
        column = across.T
        place = jnp.sum(jnp.where(column < across, 1, 0), axis=0, keepdims=True)
        hit = jnp.broadcast_to(place, (nblk, nblk)).T == lane
        order = jnp.sum(jnp.where(hit, slot, 0), axis=0, keepdims=True)
        block = jnp.sum(jnp.where(hit, column, 0), axis=0, keepdims=True) - me * local
        order = jnp.clip(order, 0, nblk - 1)
        order_v[t, pl.ds(0, 1), :] = order
        order_v[t, pl.ds(1, 1), :] = jnp.clip(block, 0, local - 1)
        order_copy(t).start()
        return order, column

    def rank_local(t, column):
        col = jnp.broadcast_to(column[:, :1], (nblk, wide))
        below = jnp.sum(jnp.where(col < own_block, 1, 0), axis=0, keepdims=True) - me * per
        found = jnp.sum(jnp.where(col == own_block, 1, 0), axis=0, keepdims=True)
        code_v[t, pl.ds(0, 1), :] = jnp.where(found > 0, jnp.clip(below, 0, per - 1), -1)
        code_copy(t).start()

    ids_copy.wait()
    first_order, column = rank_blocks(0)

    def axes(p):
        return (inner, outer) if p % 2 == 0 else (outer, inner)

    def rank(p, f, s):
        if p % 2 == 0:
            return lax.rem(y + s, outer) * inner + lax.rem(x + f, inner)
        return lax.rem(y + f, outer) * inner + lax.rem(x + s, inner)

    def span(p):
        t, start, n = pieces[p]
        return pl.ds(t * per + start, n)

    def mine(t, owner, i):
        where = lanes(order_s[t, 0, owner * per + i])
        return jnp.concatenate([part[:, where].astype(jnp.float32) for part in g[t]], axis=0)

    def first_copy(p, f, s):
        here = arrived.at[f - 1, span(p)] if s == 0 else landed.at[f - 1, s - 1, span(p)]
        return pltpu.make_async_remote_copy(
            packed.at[f - 1, s, span(p)], here, send_sem.at[0], own_sem.at[p] if s == 0 else far_sem.at[p],
            device_id={"rep": rank(p, f, 0)}, device_id_type=MESH)

    def second_copy(p, s):
        nf = axes(p)[0]
        return pltpu.make_async_remote_copy(
            relayed.at[s - 1, span(p)], arrived.at[nf - 2 + s, span(p)], send_sem.at[1], own_sem.at[p],
            device_id={"rep": rank(p, 0, s)}, device_id_type=MESH)

    def square_slot(p):
        t = pieces[p][0]
        return t if t < ntab - 1 else t + sum(q[0] == t for q in pieces[:p])

    def square_copy(p, f):
        return pltpu.make_async_remote_copy(
            sq[p].at[my_col], sq[p].at[my_col], send_sem.at[2], sq_sem.at[square_slot(p)],
            device_id={"col": lax.rem(my_col + f, cols)}, device_id_type=MESH)

    def wait_all(ref, sem):
        pltpu.make_async_copy(ref, ref, sem).wait()

    def pack(p, f, s):
        t, start, n = pieces[p]
        owner = rank(p, f, s)
        for i in range(n):
            packed[f - 1, s, t * per + start + i] = mine(t, owner, start + i)
        first_copy(p, f, s).start()

    beside_me = (y * inner + lax.rem(x + 1, inner), lax.rem(y + 1, outer) * inner + x)
    across_me = lax.rem(y + 1, outer) * inner + lax.rem(x + 1, inner)

    def way(p, owner):
        return jnp.where(owner == 1, 0, jnp.where(owner == inner, 1, p % 2))

    def steered_far(p):
        t, start, n = pieces[p]
        first = way(p, across_me)
        for i in range(n):
            packed[0, 1, t * per + start + i] = mine(t, across_me, start + i)
        b = p - first_steered
        pltpu.make_async_remote_copy(
            packed.at[0, 1, span(p)], spare.at[first, b], send_sem.at[0], spare_sem.at[first, b],
            device_id={"rep": jnp.where(first == 0, beside_me[0], beside_me[1])}, device_id_type=MESH).start()

    def steered_send(p, d, relaying):
        t, start, n = pieces[p]
        owner, b = beside_me[d], p - first_steered
        out = packed.at[0, 0] if d == 0 else relayed.at[0]

        def send():
            if relaying:
                wait_all(spare.at[1 - d, b], spare_sem.at[1 - d, b])
            for i in range(n):
                acc = mine(t, owner, start + i)
                if relaying:
                    acc = acc + spare[1 - d, b, i]
                out[t * per + start + i] = acc
            pltpu.make_async_remote_copy(
                out.at[span(p)], arrived.at[d, span(p)], send_sem.at[d], own_sem.at[p],
                device_id={"rep": owner}, device_id_type=MESH).start()

        pl.when((way(p, owner) != d) if relaying else (way(p, owner) == d))(send)

    def first_far(p, picked, h):
        t, start, n = pieces[p]
        nf, ns = axes(p)
        dims = pl.ds(h * half, half)
        for s in range(1, ns):
            for f in range(1, nf):
                for i in range(n):
                    block = g[t][h][:, lanes(picked[f, s][i])].astype(jnp.float32)
                    packed[f - 1, s, t * per + start + i, dims] = block
                pltpu.make_async_remote_copy(
                    packed.at[f - 1, s, span(p), dims], landed.at[f - 1, s - 1, span(p), dims],
                    send_sem.at[0], far_sem.at[p], device_id={"rep": rank(p, f, 0)}, device_id_type=MESH).start()

    def pick(p):
        _, start, n = pieces[p]
        nf, ns = axes(p)
        picked = {}
        for s in range(1, ns):
            for f in range(1, nf):
                row = pltpu.roll(first_order, lax.rem(nblk - rank(p, f, s) * per, nblk), 1)
                picked[f, s] = [row[0, start + i] for i in range(n)]
        return picked

    def send_far(p):
        if p >= first_steered:
            steered_far(p)
            return
        nf, ns = axes(p)
        for s in range(1, ns):
            for f in range(1, nf):
                pack(p, f, s)

    def send_near(p):
        if p >= first_steered:
            for d in range(2):
                steered_send(p, d, False)
            return
        for f in range(1, axes(p)[0]):
            pack(p, f, 0)

    def relay(p):
        if p >= first_steered:
            for d in range(2):
                steered_send(p, d, True)
            return
        t, start, n = pieces[p]
        nf, ns = axes(p)
        wait_all(landed.at[pl.ds(0, nf - 1), pl.ds(0, ns - 1), span(p)], far_sem.at[p])
        for s in range(1, ns):
            owner = rank(p, 0, s)
            for i in range(n):
                acc = mine(t, owner, start + i)
                for f in range(1, nf):
                    acc = acc + landed[f - 1, s - 1, t * per + start + i]
                relayed[s - 1, t * per + start + i] = acc
            second_copy(p, s).start()

    def finish(p):
        t, start, n = pieces[p]
        nf, ns = axes(p)
        wait_all(arrived.at[pl.ds(0, nf + ns - 2), span(p)], own_sem.at[p])
        for i in range(n):
            acc = mine(t, me, start + i)
            for k in range(nf + ns - 2):
                acc = acc + arrived[k, t * per + start + i]
            totals[t][start + i] = acc
            sq[p][my_col, pl.ds(i, 1), :] = jnp.sum(acc * acc, axis=0, keepdims=True)
        for f in range(1, cols):
            square_copy(p, f).start()

    def gather(p):
        t, start, n = pieces[p]
        if t == ntab - 1:
            wait_all(sq[p].at[pl.ds(0, cols - 1)], sq_sem.at[square_slot(p)])
        elif start == 0:
            wait_all(sent.at[:, pl.ds(0, per)], sq_sem.at[square_slot(p)])
        acc = sq[p][0]
        for f in range(1, cols):
            acc = acc + sq[p][f]
        fresh = acc_slot[t, pl.ds(start, n), :] + acc * (1.0 / dim)
        acc_slot[t, pl.ds(start, n), :] = fresh
        step[t, pl.ds(start, n), :] = 0.1 / (jnp.sqrt(fresh) + 1e-8)
        for i in range(start, start + n):
            totals[t][i] = totals[t][i] * step[t, pl.ds(i, 1), :]

    def place(t, first, end):
        for b in range(first, min(local, local - per + end)):
            code = code_s[t, 0, b]
            at = jnp.maximum(code, 0)
            where = pl.ds(b * BLOCK, BLOCK)
            spread = jnp.full((width, BLOCK), code, jnp.int32)
            hit = (spread >= first) & (spread < end) if end < per else spread >= first
            old = image[t, :, where]
            image[t, :, where] = jnp.where(hit, old - totals[t][at], old)
            old_acc = new_acc[pl.ds(t, 1), where]
            new_acc[pl.ds(t, 1), where] = jnp.where(hit[:1], acc_slot[t, pl.ds(at, 1), :], old_acc)

    def sweep(sem, way, behind, ahead):
        pl.when(behind)(lambda: pl.semaphore_wait(sem, 1))
        pl.when(ahead)(lambda: pass_on(sem, way))

    picked = [pick(p) for p in range(2)]
    beside = jnp.minimum(my_col, 1) + jnp.minimum(cols - 1 - my_col, 1)
    pl.semaphore_wait(barrier, inner - 1 + outer - 1 + beside)
    for h in range(2):
        grad_copies[0][h].wait()
        for p in range(2):
            first_far(p, picked[p], h)
    for copy in [*sum(grad_copies[1:], []), acc_copy, table_copy]:
        copy.start()
    for t in range(ntab):
        if t > 0:
            for copy in grad_copies[t]:
                copy.wait()
        order_copy(t).wait()
        for p in range(2, n_pieces):
            if pieces[p][0] == t:
                send_far(p)
        rank_local(t, column)
        if t + 1 < ntab:
            column = rank_blocks(t + 1)[1]
    for p in range(n_pieces):
        send_near(p)

    acc_copy.wait()
    for t in range(ntab):
        for i in range(per):
            block = order_s[t, 1, me * per + i]
            acc_slot[t, pl.ds(i, 1), :] = new_acc[pl.ds(t, 1), lanes(block)]

    for p in range(n_pieces):
        relay(p)
    sweep(up, 1, my_col > 0, my_col < cols - 1)
    sweep(down, -1, my_col < cols - 1, my_col > 0)
    table_copy.wait()
    wait_all(code_v, meta_sem.at[ntab])
    for p in range(n_pieces):
        finish(p)
    placed = 0
    for p in range(n_pieces):
        gather(p)
        t, start, n = pieces[p]
        if start + n == per or p == n_pieces - 3:
            place(t, placed, start + n)
            placed = 0 if start + n == per else start + n

    if inner == outer:
        wait_all(packed, send_sem.at[0])
        wait_all(relayed, send_sem.at[1])
    else:
        for p in range(n_pieces):
            nf, ns = axes(p)
            wait_all(packed.at[pl.ds(0, nf - 1), pl.ds(0, ns), span(p)], send_sem.at[0])
            wait_all(relayed.at[pl.ds(0, ns - 1), span(p)], send_sem.at[1])
    wait_all(sent, send_sem.at[2])


def store_kernel(image, acc, tables_out, acc_out, sem, acc_sem):
    copies = [pltpu.make_async_copy(acc, acc_out, acc_sem)]
    for t in range(image.shape[0]):
        copies.append(pltpu.make_async_copy(image.at[t], tables_out.at[t], sem.at[t]))
    for copy in copies:
        copy.start()
    for copy in copies:
        copy.wait()


def body(mesh, tables, accumulator, replica_grads, block_ids):
    cfg = layout(mesh, tables.shape, replica_grads.shape[3])
    ntab, width, per, nblk = cfg["ntab"], cfg["width"], cfg["per"], cfg["nblk"]
    cols, pieces = cfg["cols"], cfg["pieces"]
    side = max(cfg["inner"], cfg["outer"])
    slots, n_pieces = ntab * per, len(pieces)
    wide = -(-cfg["local"] // BLOCK) * BLOCK
    f32, i32 = jnp.float32, jnp.int32
    dma = pltpu.SemaphoreType.DMA
    hbm = pl.BlockSpec(memory_space=pltpu.HBM)
    vmem = pl.BlockSpec(memory_space=pltpu.VMEM)
    image, new_acc = pl.pallas_call(
        functools.partial(step_kernel, cfg),
        out_shape=(jax.ShapeDtypeStruct(tables.shape, f32), jax.ShapeDtypeStruct(accumulator.shape, f32)),
        in_specs=[hbm] * 4,
        out_specs=(vmem, vmem),
        scratch_shapes=[
            *[pltpu.VMEM((width // 2, replica_grads.shape[3]), replica_grads.dtype) for _ in range(2 * ntab)],
            *[pltpu.VMEM((per, width, BLOCK), f32) for _ in range(ntab)],
            *[pltpu.VMEM((cols, n, BLOCK), f32) for _, _, n in pieces],
            pltpu.VMEM(block_ids.shape, i32),
            pltpu.VMEM((ntab, 2, nblk), i32),
            pltpu.VMEM((ntab, 1, wide), i32),
            pltpu.SMEM((ntab, 2, nblk), i32),
            pltpu.SMEM((ntab, 1, wide), i32),
            pltpu.VMEM((side - 1, side, slots, width, BLOCK), f32),
            pltpu.VMEM((side - 1, side - 1, slots, width, BLOCK), f32),
            pltpu.VMEM((side - 1, slots, width, BLOCK), f32),
            pltpu.VMEM((2 * side - 2, slots, width, BLOCK), f32),
            pltpu.VMEM((ntab, per, BLOCK), f32),
            pltpu.VMEM((ntab, per, BLOCK), f32),
            pltpu.VMEM((cols - 1, slots, BLOCK), f32),
            pltpu.VMEM((2, 2, pieces[-1][2], width, BLOCK), f32),
            dma((3 + 2 * ntab,)), dma((ntab + 1,)), dma((3,)),
            dma((n_pieces - cfg["steered"],)), dma((n_pieces,)), dma((ntab - 1 + sum(q[0] == ntab - 1 for q in pieces),)),
            pltpu.SemaphoreType.REGULAR, pltpu.SemaphoreType.REGULAR, dma((2, 2)),
        ],
        compiler_params=pltpu.CompilerParams(
            collective_id=0, has_side_effects=True, vmem_limit_bytes=32 * 2**20),
        name="exchange",
    )(*[pltpu.with_memory_space_constraint(a, pltpu.HBM) for a in (block_ids, replica_grads, tables, accumulator)])
    return pl.pallas_call(
        store_kernel,
        out_shape=(jax.ShapeDtypeStruct(tables.shape, f32), jax.ShapeDtypeStruct(accumulator.shape, f32)),
        in_specs=[vmem, vmem],
        out_specs=(hbm, hbm),
        scratch_shapes=[dma((ntab,)), dma(())],
        compiler_params=pltpu.CompilerParams(vmem_limit_bytes=2**20),
        name="store",
    )(image, new_acc)


def solution(mesh):
    return jax.shard_map(
        functools.partial(body, mesh),
        mesh=mesh,
        in_specs=(P(None, "col", "rep"), P(None, "rep"), P("rep", None, "col", None), P()),
        out_specs=(P(None, "col", "rep"), P(None, "rep")),
        check_vma=False,
    )
```

```python
import functools
import math

import jax
import jax.numpy as jnp
from jax import lax
from jax.experimental import pallas as pl
from jax.experimental.pallas import tpu as pltpu
from jax.sharding import PartitionSpec as P

BLOCK = 128
MESH = pl.DeviceIdType.MESH


def cuts(per, last):
    if per % 8:
        return [1] * per
    unit = per // 8
    tail = max(1, 3 * unit // 4)
    return [2 * unit] * 2 + [2 * unit - tail] * 2 + [tail] * 2 if last else [unit] * 2 + [3 * unit] * 2


def layout(mesh, shape, n_slab):
    reps, cols = mesh.shape["rep"], mesh.shape["col"]
    inner = math.isqrt(reps)
    while reps % inner:
        inner -= 1
    ntab, width, local_rows = shape
    per = n_slab // BLOCK // reps
    pieces = []
    for t in range(ntab):
        start = 0
        for n in cuts(per, t == ntab - 1):
            pieces.append((t, start, n))
            start += n
    steered = 2 if inner == 2 and reps == 4 else 0
    return dict(steered=steered, reps=reps, cols=cols, inner=inner, outer=reps // inner, ntab=ntab, width=width,
                per=per, nblk=n_slab // BLOCK, local=local_rows // BLOCK, dim=width * cols, pieces=pieces)


def lanes(i):
    return pl.ds(i * BLOCK, BLOCK)


def step_kernel(cfg, ids_hbm, grads_hbm, tables_hbm, acc_hbm, image, new_acc, *scratch):
    reps, cols, inner, outer = cfg["reps"], cfg["cols"], cfg["inner"], cfg["outer"]
    ntab, width, per, nblk = cfg["ntab"], cfg["width"], cfg["per"], cfg["nblk"]
    local, dim, pieces = cfg["local"], cfg["dim"], cfg["pieces"]
    n_pieces = len(pieces)
    scratch = list(scratch)

    def take(n):
        out = scratch[:n]
        del scratch[:n]
        return out

    g = [take(2) for _ in range(ntab)]
    totals = take(ntab)
    half = width // 2
    sq = take(n_pieces)
    (ids_v, order_v, code_v, order_s, code_s, packed, landed, relayed, arrived, acc_slot, step, sent, spare,
     in_sem, meta_sem, send_sem, far_sem, own_sem, sq_sem, up, down, spare_sem) = scratch
    first_steered = n_pieces - cfg["steered"]

    me = lax.axis_index("rep")
    my_col = lax.axis_index("col")
    x, y = lax.rem(me, inner), me // inner

    ids_copy = pltpu.make_async_copy(ids_hbm, ids_v, in_sem.at[0])
    ids_copy.start()
    grad_copies = [[pltpu.make_async_copy(grads_hbm.at[0, t, pl.ds(h * half, half)], g[t][h], in_sem.at[3 + 2 * t + h])
                    for h in range(2)] for t in range(ntab)]
    for copy in grad_copies[0]:
        copy.start()

    barrier = pltpu.get_barrier_semaphore()
    for f in range(1, inner):
        pl.semaphore_signal(barrier, inc=1, device_id={"rep": y * inner + lax.rem(x + f, inner)}, device_id_type=MESH)
    for f in range(1, outer):
        pl.semaphore_signal(barrier, inc=1, device_id={"rep": lax.rem(y + f, outer) * inner + x}, device_id_type=MESH)

    def pass_on(sem, way):
        pl.semaphore_signal(sem, inc=1, device_id={"col": my_col + way}, device_id_type=MESH)

    pl.when(my_col > 0)(lambda: pass_on(barrier, -1))
    pl.when(my_col < cols - 1)(lambda: pass_on(barrier, 1))

    acc_copy = pltpu.make_async_copy(acc_hbm, new_acc, in_sem.at[1])
    table_copy = pltpu.make_async_copy(tables_hbm, image, in_sem.at[2])

    lane = lax.broadcasted_iota(jnp.int32, (nblk, nblk), 1)
    slot = lax.broadcasted_iota(jnp.int32, (nblk, nblk), 0)
    wide = code_v.shape[2]
    own_block = lax.broadcasted_iota(jnp.int32, (nblk, wide), 1) + me * local

    def order_copy(t):
        return pltpu.make_async_copy(order_v.at[t], order_s.at[t], meta_sem.at[t])

    def code_copy(t):
        return pltpu.make_async_copy(code_v.at[t], code_s.at[t], meta_sem.at[ntab])

    def rank_blocks(t):
        across = jnp.broadcast_to(ids_v[pl.ds(t, 1), :], (nblk, nblk))
        column = across.T
        place = jnp.sum(jnp.where(column < across, 1, 0), axis=0, keepdims=True)
        hit = jnp.broadcast_to(place, (nblk, nblk)).T == lane
        order = jnp.sum(jnp.where(hit, slot, 0), axis=0, keepdims=True)
        block = jnp.sum(jnp.where(hit, column, 0), axis=0, keepdims=True) - me * local
        order = jnp.clip(order, 0, nblk - 1)
        order_v[t, pl.ds(0, 1), :] = order
        order_v[t, pl.ds(1, 1), :] = jnp.clip(block, 0, local - 1)
        order_copy(t).start()
        return order, column

    def rank_local(t, column):
        col = jnp.broadcast_to(column[:, :1], (nblk, wide))
        below = jnp.sum(jnp.where(col < own_block, 1, 0), axis=0, keepdims=True) - me * per
        found = jnp.sum(jnp.where(col == own_block, 1, 0), axis=0, keepdims=True)
        code_v[t, pl.ds(0, 1), :] = jnp.where(found > 0, jnp.clip(below, 0, per - 1), -1)
        code_copy(t).start()

    ids_copy.wait()
    first_order, column = rank_blocks(0)

    def axes(p):
        return (inner, outer) if p % 2 == 0 else (outer, inner)

    def rank(p, f, s):
        if p % 2 == 0:
            return lax.rem(y + s, outer) * inner + lax.rem(x + f, inner)
        return lax.rem(y + f, outer) * inner + lax.rem(x + s, inner)

    def span(p):
        t, start, n = pieces[p]
        return pl.ds(t * per + start, n)

    def mine(t, owner, i):
        where = lanes(order_s[t, 0, owner * per + i])
        return jnp.concatenate([part[:, where].astype(jnp.float32) for part in g[t]], axis=0)

    def first_copy(p, f, s):
        here = arrived.at[f - 1, span(p)] if s == 0 else landed.at[f - 1, s - 1, span(p)]
        return pltpu.make_async_remote_copy(
            packed.at[f - 1, s, span(p)], here, send_sem.at[0], own_sem.at[own_slot(p)] if s == 0 else far_sem.at[p],
            device_id={"rep": rank(p, f, 0)}, device_id_type=MESH)

    def second_copy(p, s):
        nf = axes(p)[0]
        return pltpu.make_async_remote_copy(
            relayed.at[s - 1, span(p)], arrived.at[nf - 2 + s, span(p)], send_sem.at[1], own_sem.at[own_slot(p)],
            device_id={"rep": rank(p, 0, s)}, device_id_type=MESH)

    def square_slot(p):
        t = pieces[p][0]
        return t if t < ntab - 1 else t + sum(q[0] == t for q in pieces[:p])

    def own_slot(p):
        return square_slot(p) if inner == outer else p

    def square_copy(p, f):
        return pltpu.make_async_remote_copy(
            sq[p].at[my_col], sq[p].at[my_col], send_sem.at[2], sq_sem.at[square_slot(p)],
            device_id={"col": lax.rem(my_col + f, cols)}, device_id_type=MESH)

    def wait_all(ref, sem):
        pltpu.make_async_copy(ref, ref, sem).wait()

    def pack(p, f, s):
        t, start, n = pieces[p]
        owner = rank(p, f, s)
        for i in range(n):
            packed[f - 1, s, t * per + start + i] = mine(t, owner, start + i)
        first_copy(p, f, s).start()

    beside_me = (y * inner + lax.rem(x + 1, inner), lax.rem(y + 1, outer) * inner + x)
    across_me = lax.rem(y + 1, outer) * inner + lax.rem(x + 1, inner)

    def way(p, owner):
        return jnp.where(owner == 1, 0, jnp.where(owner == inner, 1, p % 2))

    def steered_far(p):
        t, start, n = pieces[p]
        first = way(p, across_me)
        for i in range(n):
            packed[0, 1, t * per + start + i] = mine(t, across_me, start + i)
        b = p - first_steered
        pltpu.make_async_remote_copy(
            packed.at[0, 1, span(p)], spare.at[first, b], send_sem.at[0], spare_sem.at[first, b],
            device_id={"rep": jnp.where(first == 0, beside_me[0], beside_me[1])}, device_id_type=MESH).start()

    def steered_send(p, d, relaying):
        t, start, n = pieces[p]
        owner, b = beside_me[d], p - first_steered
        out = packed.at[0, 0] if d == 0 else relayed.at[0]

        def send():
            if relaying:
                wait_all(spare.at[1 - d, b], spare_sem.at[1 - d, b])
            for i in range(n):
                acc = mine(t, owner, start + i)
                if relaying:
                    acc = acc + spare[1 - d, b, i]
                out[t * per + start + i] = acc
            pltpu.make_async_remote_copy(
                out.at[span(p)], arrived.at[d, span(p)], send_sem.at[d], own_sem.at[own_slot(p)],
                device_id={"rep": owner}, device_id_type=MESH).start()

        pl.when((way(p, owner) != d) if relaying else (way(p, owner) == d))(send)

    def first_far(p, picked, h):
        t, start, n = pieces[p]
        nf, ns = axes(p)
        dims = pl.ds(h * half, half)
        for s in range(1, ns):
            for f in range(1, nf):
                for i in range(n):
                    block = g[t][h][:, lanes(picked[f, s][i])].astype(jnp.float32)
                    packed[f - 1, s, t * per + start + i, dims] = block
                pltpu.make_async_remote_copy(
                    packed.at[f - 1, s, span(p), dims], landed.at[f - 1, s - 1, span(p), dims],
                    send_sem.at[0], far_sem.at[p], device_id={"rep": rank(p, f, 0)}, device_id_type=MESH).start()

    def pick(p):
        _, start, n = pieces[p]
        nf, ns = axes(p)
        picked = {}
        for s in range(1, ns):
            for f in range(1, nf):
                row = pltpu.roll(first_order, lax.rem(nblk - rank(p, f, s) * per, nblk), 1)
                picked[f, s] = [row[0, start + i] for i in range(n)]
        return picked

    def send_far(p):
        if p >= first_steered:
            steered_far(p)
            return
        nf, ns = axes(p)
        for s in range(1, ns):
            for f in range(1, nf):
                pack(p, f, s)

    def send_near(p):
        if p >= first_steered:
            for d in range(2):
                steered_send(p, d, False)
            return
        for f in range(1, axes(p)[0]):
            pack(p, f, 0)

    def relay(p):
        if p >= first_steered:
            for d in range(2):
                steered_send(p, d, True)
            return
        t, start, n = pieces[p]
        nf, ns = axes(p)
        wait_all(landed.at[pl.ds(0, nf - 1), pl.ds(0, ns - 1), span(p)], far_sem.at[p])
        for s in range(1, ns):
            owner = rank(p, 0, s)
            for i in range(n):
                acc = mine(t, owner, start + i)
                for f in range(1, nf):
                    acc = acc + landed[f - 1, s - 1, t * per + start + i]
                relayed[s - 1, t * per + start + i] = acc
            second_copy(p, s).start()

    def finish(p):
        t, start, n = pieces[p]
        nf, ns = axes(p)
        if t == ntab - 1 or inner != outer:
            wait_all(arrived.at[pl.ds(0, nf + ns - 2), span(p)], own_sem.at[own_slot(p)])
        elif start == 0:
            wait_all(arrived.at[pl.ds(0, nf + ns - 2), pl.ds(t * per, per)], own_sem.at[own_slot(p)])
        for i in range(n):
            acc = mine(t, me, start + i)
            for k in range(nf + ns - 2):
                acc = acc + arrived[k, t * per + start + i]
            totals[t][start + i] = acc
            sq[p][my_col, pl.ds(i, 1), :] = jnp.sum(acc * acc, axis=0, keepdims=True)
        for f in range(1, cols):
            square_copy(p, f).start()

    def gather(p):
        t, start, n = pieces[p]
        if t == ntab - 1:
            wait_all(sq[p].at[pl.ds(0, cols - 1)], sq_sem.at[square_slot(p)])
        elif start == 0:
            wait_all(sent.at[:, pl.ds(0, per)], sq_sem.at[square_slot(p)])
        acc = sq[p][0]
        for f in range(1, cols):
            acc = acc + sq[p][f]
        fresh = acc_slot[t, pl.ds(start, n), :] + acc * (1.0 / dim)
        acc_slot[t, pl.ds(start, n), :] = fresh
        step[t, pl.ds(start, n), :] = 0.1 / (jnp.sqrt(fresh) + 1e-8)
        for i in range(start, start + n):
            totals[t][i] = totals[t][i] * step[t, pl.ds(i, 1), :]

    def place(t, first, end):
        for b in range(first, min(local, local - per + end)):
            code = code_s[t, 0, b]
            at = jnp.maximum(code, 0)
            where = pl.ds(b * BLOCK, BLOCK)
            spread = jnp.full((width, BLOCK), code, jnp.int32)
            hit = (spread >= first) & (spread < end) if end < per else spread >= first
            old = image[t, :, where]
            image[t, :, where] = jnp.where(hit, old - totals[t][at], old)
            old_acc = new_acc[pl.ds(t, 1), where]
            new_acc[pl.ds(t, 1), where] = jnp.where(hit[:1], acc_slot[t, pl.ds(at, 1), :], old_acc)

    def sweep(sem, way, behind, ahead):
        pl.when(behind)(lambda: pl.semaphore_wait(sem, 1))
        pl.when(ahead)(lambda: pass_on(sem, way))

    picked = [pick(p) for p in range(2)]
    beside = jnp.minimum(my_col, 1) + jnp.minimum(cols - 1 - my_col, 1)
    pl.semaphore_wait(barrier, inner - 1 + outer - 1 + beside)
    for h in range(2):
        grad_copies[0][h].wait()
        for p in range(2):
            first_far(p, picked[p], h)
    for copy in [*sum(grad_copies[1:], []), acc_copy, table_copy]:
        copy.start()
    for t in range(ntab):
        if t > 0:
            for copy in grad_copies[t]:
                copy.wait()
        order_copy(t).wait()
        for p in range(2, n_pieces):
            if pieces[p][0] == t:
                send_far(p)
        rank_local(t, column)
        if t + 1 < ntab:
            column = rank_blocks(t + 1)[1]
    for p in range(n_pieces):
        send_near(p)

    acc_copy.wait()
    for t in range(ntab):
        for i in range(per):
            block = order_s[t, 1, me * per + i]
            acc_slot[t, pl.ds(i, 1), :] = new_acc[pl.ds(t, 1), lanes(block)]

    for p in range(n_pieces):
        relay(p)
    sweep(up, 1, my_col > 0, my_col < cols - 1)
    sweep(down, -1, my_col < cols - 1, my_col > 0)
    table_copy.wait()
    wait_all(code_v, meta_sem.at[ntab])
    for p in range(n_pieces):
        finish(p)
    placed = 0
    for p in range(n_pieces):
        gather(p)
        t, start, n = pieces[p]
        if start + n == per or p == n_pieces - 3:
            place(t, placed, start + n)
            placed = 0 if start + n == per else start + n

    if inner == outer:
        wait_all(packed, send_sem.at[0])
        wait_all(relayed, send_sem.at[1])
    else:
        for p in range(n_pieces):
            nf, ns = axes(p)
            wait_all(packed.at[pl.ds(0, nf - 1), pl.ds(0, ns), span(p)], send_sem.at[0])
            wait_all(relayed.at[pl.ds(0, ns - 1), span(p)], send_sem.at[1])
    wait_all(sent, send_sem.at[2])


def store_kernel(image, acc, tables_out, acc_out, sem, acc_sem):
    copies = [pltpu.make_async_copy(acc, acc_out, acc_sem)]
    for t in range(image.shape[0]):
        copies.append(pltpu.make_async_copy(image.at[t], tables_out.at[t], sem.at[t]))
    for copy in copies:
        copy.start()
    for copy in copies:
        copy.wait()


def body(mesh, tables, accumulator, replica_grads, block_ids):
    cfg = layout(mesh, tables.shape, replica_grads.shape[3])
    ntab, width, per, nblk = cfg["ntab"], cfg["width"], cfg["per"], cfg["nblk"]
    cols, pieces = cfg["cols"], cfg["pieces"]
    side = max(cfg["inner"], cfg["outer"])
    slots, n_pieces = ntab * per, len(pieces)
    few = ntab - 1 + sum(q[0] == ntab - 1 for q in pieces)
    wide = -(-cfg["local"] // BLOCK) * BLOCK
    f32, i32 = jnp.float32, jnp.int32
    dma = pltpu.SemaphoreType.DMA
    hbm = pl.BlockSpec(memory_space=pltpu.HBM)
    vmem = pl.BlockSpec(memory_space=pltpu.VMEM)
    image, new_acc = pl.pallas_call(
        functools.partial(step_kernel, cfg),
        out_shape=(jax.ShapeDtypeStruct(tables.shape, f32), jax.ShapeDtypeStruct(accumulator.shape, f32)),
        in_specs=[hbm] * 4,
        out_specs=(vmem, vmem),
        scratch_shapes=[
            *[pltpu.VMEM((width // 2, replica_grads.shape[3]), replica_grads.dtype) for _ in range(2 * ntab)],
            *[pltpu.VMEM((per, width, BLOCK), f32) for _ in range(ntab)],
            *[pltpu.VMEM((cols, n, BLOCK), f32) for _, _, n in pieces],
            pltpu.VMEM(block_ids.shape, i32),
            pltpu.VMEM((ntab, 2, nblk), i32),
            pltpu.VMEM((ntab, 1, wide), i32),
            pltpu.SMEM((ntab, 2, nblk), i32),
            pltpu.SMEM((ntab, 1, wide), i32),
            pltpu.VMEM((side - 1, side, slots, width, BLOCK), f32),
            pltpu.VMEM((side - 1, side - 1, slots, width, BLOCK), f32),
            pltpu.VMEM((side - 1, slots, width, BLOCK), f32),
            pltpu.VMEM((2 * side - 2, slots, width, BLOCK), f32),
            pltpu.VMEM((ntab, per, BLOCK), f32),
            pltpu.VMEM((ntab, per, BLOCK), f32),
            pltpu.VMEM((cols - 1, slots, BLOCK), f32),
            pltpu.VMEM((2, 2, pieces[-1][2], width, BLOCK), f32),
            dma((3 + 2 * ntab,)), dma((ntab + 1,)), dma((3,)),
            dma((n_pieces - cfg["steered"],)), dma((few if cfg["inner"] == cfg["outer"] else n_pieces,)), dma((few,)),
            pltpu.SemaphoreType.REGULAR, pltpu.SemaphoreType.REGULAR, dma((2, 2)),
        ],
        compiler_params=pltpu.CompilerParams(
            collective_id=0, has_side_effects=True, vmem_limit_bytes=32 * 2**20),
        name="exchange",
    )(*[pltpu.with_memory_space_constraint(a, pltpu.HBM) for a in (block_ids, replica_grads, tables, accumulator)])
    return pl.pallas_call(
        store_kernel,
        out_shape=(jax.ShapeDtypeStruct(tables.shape, f32), jax.ShapeDtypeStruct(accumulator.shape, f32)),
        in_specs=[vmem, vmem],
        out_specs=(hbm, hbm),
        scratch_shapes=[dma((ntab,)), dma(())],
        compiler_params=pltpu.CompilerParams(vmem_limit_bytes=2**20),
        name="store",
    )(image, new_acc)


def solution(mesh):
    return jax.shard_map(
        functools.partial(body, mesh),
        mesh=mesh,
        in_specs=(P(None, "col", "rep"), P(None, "rep"), P("rep", None, "col", None), P()),
        out_specs=(P(None, "col", "rep"), P(None, "rep")),
        check_vma=False,
    )
```
